32 devices in a mesh: row: 8 (over y, x, core), col: 4 (over z).
Axes of the slice: x: 2, y: 2, z: 4, core: 2. Of those that a mesh axis runs over, the one named last changes fastest.
Arguments:
- features: bfloat16 [65536, 256], P(('col', 'row')), may hold values from -6 to 6
- block_values: bfloat16 [8, 4, 192, 128, 128], P('row', 'col'), may hold values from -0.1875 to 0.1875
- row_ptr: int32 [8, 4, 65], P('row', 'col'), may hold values from 0 to 144, as said below
- block_cols: int32 [8, 4, 192], P('row', 'col'), may hold values from 0 to 511, as said below
Outputs:
- product: bfloat16 [65536, 256], P(('row', 'col'))
The draws below stay inside these ranges and needn't reach their ends.
Inputs may be any that keep to these rules, and one draw needn't show every extreme that they name: row_ptr[r, c, 0] = 0, row_ptr never falls along its last dimension, row_ptr[r, c, 64] <= 144, and on exactly one device row_ptr[r, c, 64] = 144. block_cols[r, c, s] lies in c * 128 to (c + 1) * 128 - 1; a block column may repeat within a block row, and repeated blocks add.
All inputs are finite; a program needn't handle non-finite values.
Results may differ from the reference program's by a relative error of at most 0.001.
Values may be sent and summed in bfloat16 or wider, within the bound.
No kernel may reach another device: no remote copies, remote signals or barrier semaphores. Data moves between devices by JAX's collectives and lax.ppermute only.
A program may use at most 128 MiB of HBM per device.

```python
import jax
import jax.numpy as jnp
from jax import lax

B = 128
NCOL = 256
BR = 64
SLOTS = 192
NB = 512
BC = 128
N_ROW = 8
N_COL = 4


def pattern(key):
    key_fill = jax.random.fold_in(key, 11)
    key_busy = jax.random.fold_in(key, 12)
    key_rows = jax.random.fold_in(key, 13)
    key_cols = jax.random.fold_in(key, 14)
    filled = SLOTS // 8 + jax.random.randint(key_fill, (N_ROW, N_COL), 0, SLOTS // 4 + 1)
    busiest = jax.random.randint(key_busy, (), 0, N_ROW * N_COL)
    position = jnp.arange(N_ROW * N_COL, dtype=jnp.int32).reshape(N_ROW, N_COL)
    filled = jnp.where(position == busiest, 3 * SLOTS // 4, filled)
    slot_ids = jnp.arange(SLOTS, dtype=jnp.int32)
    rows = jax.random.randint(key_rows, (N_ROW, N_COL, SLOTS), 0, BR)
    rows = jnp.where(slot_ids[None, None, :] < filled[:, :, None], rows, BR)
    bounds = jnp.arange(BR + 1, dtype=jnp.int32)
    pointers = jnp.sum((rows[:, :, None, :] < bounds[None, None, :, None]).astype(jnp.int32), axis=-1)
    group_start = (jnp.arange(N_COL, dtype=jnp.int32) * BC)[None, :, None]
    columns = jax.random.randint(key_cols, (N_ROW, N_COL, SLOTS), 0, BC) + group_start
    return (pointers.astype(jnp.int32), columns.astype(jnp.int32))


def draw_row_ptr(key, part):
    pointers, columns = pattern(key)
    return pointers


def draw_block_cols(key, part):
    pointers, columns = pattern(key)
    return columns


def level_of(rng, shape, pieces, low, top_value):
    gain = 1.0
    for dim, shards_of in pieces:
        heights = jax.random.uniform(jax.random.fold_in(jax.random.fold_in(rng, 6), dim), (shards_of,), jnp.float32, low / len(pieces), top_value / len(pieces))
        gain = gain * jnp.repeat(jnp.exp(heights), shape[dim] // shards_of).reshape((-1,) + (1,) * (len(shape) - 1 - dim))
    return gain


def scatter_about(rng, dims, scale, most, split=(), kind=jnp.bfloat16):
    array = scale * jax.random.normal(rng, dims, jnp.float32)
    if split:
        array = array * level_of(rng, dims, split, -0.22, 0.18)
    return jnp.clip(array, -most, most).astype(kind)


def setup_inputs(seed: int = 0) -> dict:
    seeds = jax.random.split(jax.random.key(seed), 5)
    features = scatter_about(seeds[0], (NB * B, NCOL), 1.0, 6.0, ((0, 32),))
    block_values = scatter_about(seeds[1], (N_ROW, N_COL, SLOTS, B, B), (9 * B) ** -0.5, 0.1875, ((0, 8), (1, 4)))
    row_ptr = draw_row_ptr(jax.random.fold_in(seeds[4], 71), 0)
    block_cols = draw_block_cols(jax.random.fold_in(seeds[4], 71), 0)
    return dict(features=features, block_values=block_values, row_ptr=row_ptr, block_cols=block_cols)


def row_weights(pointers, slot_count):
    slot_ids = jnp.arange(slot_count, dtype=jnp.int32)
    inside = (pointers[:-1, None] <= slot_ids[None, :]) & (slot_ids[None, :] < pointers[1:, None])
    return inside.astype(jnp.float32)


def reference(features, block_values, row_ptr, block_cols):
    block_size = block_values.shape[-1]
    panel = features.reshape(-1, block_size, features.shape[1])

    def one_group(operands):
        values_row, pointers_row, columns_row = operands

        def add_device(running, device_ops):
            values, pointers, columns = device_ops
            blocks = panel[columns.astype(jnp.int32)].astype(jnp.float32)
            products = jnp.einsum("sij,sjk->sik", values.astype(jnp.float32), blocks, precision=lax.Precision.HIGHEST)
            weights = row_weights(pointers.astype(jnp.int32), values.shape[0])
            summed = jnp.einsum("rs,sik->rik", weights, products, precision=lax.Precision.HIGHEST)
            return running + summed, jnp.zeros((), jnp.float32)

        starting = jnp.zeros((row_ptr.shape[2] - 1, block_size, features.shape[1]), jnp.float32)
        running, unused = lax.scan(add_device, starting, (values_row, pointers_row, columns_row))
        return running

    groups = lax.map(one_group, (block_values, row_ptr, block_cols))
    return groups.reshape(features.shape[0], features.shape[1]).astype(jnp.bfloat16)
```

```python
import functools

import jax
import jax.numpy as jnp
from jax import lax
from jax.experimental import pallas as pl
from jax.experimental.pallas import tpu as pltpu
from jax.sharding import PartitionSpec as P


LANES = 128
UNROLL = 8
TOP = 32700.0
STEPS = 8.0
TINY = 2.0**-110


def code_of(peak):
    return jnp.ceil(jnp.log2(jnp.maximum(peak, TINY)) * STEPS)


def encode(y):
    code = code_of(jnp.max(jnp.abs(y), axis=0, keepdims=True))
    coded = jnp.round(y * (jnp.exp2(code * (-1.0 / STEPS)) * TOP))
    return coded.astype(jnp.int32).astype(jnp.int16), code


def scale_of(codes):
    return jnp.exp2(codes.astype(jnp.float32) * (1.0 / STEPS)) * (1.0 / TOP)


def product_kernel(sizes, count_ref, index_ref, row_ref, owner_ref, values_ref, *refs):
    pieces, messages, block, owned, panel_rows = sizes
    piece_refs = refs[:pieces]
    out_refs = refs[pieces : pieces + messages]
    own_ref = refs[pieces + messages]
    panel, store, acc, coded, codes, piece_sem, store_sem, out_sem = refs[pieces + messages + 1 :]
    steps = (count_ref[0] + UNROLL - 1) // UNROLL

    def piece_copy(p):
        return pltpu.make_async_copy(
            piece_refs[p], panel.at[pl.ds(p * panel_rows, panel_rows)], piece_sem.at[p]
        )

    def store_copy(t):
        span = pl.ds(t * UNROLL, UNROLL)
        return pltpu.make_async_copy(values_ref.at[span], store.at[span], store_sem.at[t])

    for p in range(pieces):
        piece_copy(p).start()

    @pl.loop(0, steps)
    def _(t):
        store_copy(t).start()

    @pl.loop(0, acc.shape[0] - 1)
    def _(i):
        acc[i] = jnp.zeros(acc.shape[1:], acc.dtype)

    for p in range(pieces):
        piece_copy(p).wait()

    @pl.loop(0, steps)
    def _(t):
        store_copy(t).wait()
        terms = []
        for u in range(UNROLL):
            s = t * UNROLL + u
            x = panel[pl.ds(pl.multiple_of(index_ref[s] * block, block), block), :]
            terms.append(jnp.dot(store[s], x, preferred_element_type=jnp.float32))
        for u in range(UNROLL):
            acc[row_ref[t * UNROLL + u]] += terms[u]

    copies = []
    for m in range(messages):
        first = owner_ref[m] * owned

        @pl.loop(0, owned)
        def _(i):
            y, code = encode(acc[first + i])
            coded[m, pl.ds(pl.multiple_of(i * block, block), block), :] = y
            codes[m, pl.ds(i, 1), :] = code

        tail = codes.shape[1]
        coded[m, owned * block : owned * block + tail, :] = (
            codes[m].astype(jnp.int32).astype(jnp.int16)
        )
        copy = pltpu.make_async_copy(coded.at[m], out_refs[m], out_sem.at[m])
        copy.start()
        copies.append(copy)
    copy = pltpu.make_async_copy(
        acc.at[pl.ds(owner_ref[messages] * owned, owned)], own_ref, out_sem.at[messages]
    )
    copy.start()
    copies.append(copy)
    for copy in copies:
        copy.wait()


def products(count, index, rows, owners, values, pieces, owned, local_rows):
    block = values.shape[1]
    slots = values.shape[0]
    messages = owners.shape[0] - 1
    panel_rows, width = pieces[0].shape
    tail = -(-owned // 16) * 16
    length = owned * block + tail
    smem = pl.BlockSpec(memory_space=pltpu.SMEM)
    anywhere = pl.BlockSpec(memory_space=pl.ANY)
    flops = 2 * slots * block * block * width
    out = pl.pallas_call(
        functools.partial(
            product_kernel, (len(pieces), messages, block, owned, panel_rows)
        ),
        out_shape=[jax.ShapeDtypeStruct((length, width), jnp.int16)] * messages
        + [jax.ShapeDtypeStruct((owned, block, width), jnp.float32)],
        in_specs=[smem] * 4 + [anywhere] * (1 + len(pieces)),
        out_specs=[anywhere] * (messages + 1),
        scratch_shapes=[
            pltpu.VMEM((len(pieces) * panel_rows, width), values.dtype),
            pltpu.VMEM(values.shape, values.dtype),
            pltpu.VMEM((local_rows + 1, block, width), jnp.float32),
            pltpu.VMEM((messages, length, width), jnp.int16),
            pltpu.VMEM((messages, tail, width), jnp.float32),
            pltpu.SemaphoreType.DMA((len(pieces),)),
            pltpu.SemaphoreType.DMA((slots // UNROLL,)),
            pltpu.SemaphoreType.DMA((messages + 1,)),
        ],
        cost_estimate=pl.CostEstimate(flops=8 * flops, bytes_accessed=1 << 23, transcendentals=0),
    )(count, index, rows, owners, values, *pieces)
    return out[:messages], out[messages]


def decoded(ref, codes, i, block):
    q = ref[pl.ds(pl.multiple_of(i * block, block), block), :]
    return q.astype(jnp.int32).astype(jnp.float32) * codes[pl.ds(i, 1), :]


def merge_kernel(block, owned, *refs):
    *in_refs, out_ref, codes, new = refs
    for n, ref in enumerate(in_refs):
        codes[n] = scale_of(ref[owned * block :, :].astype(jnp.int32))

    @pl.loop(0, owned)
    def _(i):
        total = sum(decoded(ref, codes.at[n], i, block) for n, ref in enumerate(in_refs))
        y, code = encode(total)
        out_ref[pl.ds(pl.multiple_of(i * block, block), block), :] = y
        new[pl.ds(i, 1), :] = code

    out_ref[owned * block :, :] = new[...].astype(jnp.int32).astype(jnp.int16)


def merge(terms, block, owned):
    length, width = terms[0].shape
    tail = length - owned * block
    whole = pl.BlockSpec(memory_space=pltpu.VMEM)
    return pl.pallas_call(
        functools.partial(merge_kernel, block, owned),
        out_shape=jax.ShapeDtypeStruct((length, width), jnp.int16),
        in_specs=[whole] * len(terms),
        out_specs=whole,
        scratch_shapes=[
            pltpu.VMEM((len(terms), tail, width), jnp.float32),
            pltpu.VMEM((tail, width), jnp.float32),
        ],
        cost_estimate=pl.CostEstimate(
            flops=1 << 28, bytes_accessed=3 * length * width * 2, transcendentals=0
        ),
    )(*terms)


def finish_kernel(block, owned, terms, *refs):
    own_ref = refs[0]
    in_refs = refs[1 : 1 + terms]
    out_ref, codes = refs[-2:]
    for n, ref in enumerate(in_refs):
        codes[n] = scale_of(ref[owned * block :, :].astype(jnp.int32))

    @pl.loop(0, owned)
    def _(i):
        total = own_ref[i] + sum(decoded(ref, codes.at[n], i, block) for n, ref in enumerate(in_refs))
        out_ref[pl.ds(pl.multiple_of(i * block, block), block), :] = total.astype(out_ref.dtype)


def finish(own, terms):
    owned, block, width = own.shape
    length = terms[0].shape[0]
    whole = pl.BlockSpec(memory_space=pltpu.VMEM)
    return pl.pallas_call(
        functools.partial(finish_kernel, block, owned, len(terms)),
        out_shape=jax.ShapeDtypeStruct((owned * block, width), jnp.bfloat16),
        in_specs=[whole] * (1 + len(terms)),
        out_specs=whole,
        scratch_shapes=[pltpu.VMEM((len(terms), length - owned * block, width), jnp.float32)],
        cost_estimate=pl.CostEstimate(
            flops=1 << 28, bytes_accessed=4 * length * width * 2, transcendentals=0
        ),
    )(own, *terms)


def gather(part, devices):
    pieces = []
    for p in range(0, devices, 2):
        near = part if p == 0 else lax.ppermute(part, "row", [(d, d ^ p) for d in range(devices)])
        pieces += [near, lax.ppermute(near, "row", [(d, d ^ 1) for d in range(devices)])]
    return pieces


def plan(count):
    out = []
    for d in range(count - 1, 0, -1):
        right = [(z, z + d) for z in range(count - d)]
        left = [(z, z - d) for z in range(d, count)]
        out.append((d, right, left, count - 1 - d < d - 1 or (d == 2 and count == 4)))
    return out


def local(features, block_values, row_ptr, block_cols):
    values = block_values[0, 0]
    pointers = row_ptr[0, 0]
    slots, block = values.shape[:2]
    local_rows = pointers.shape[0] - 1
    row_count, col_count = lax.axis_size("row"), lax.axis_size("col")
    row, col = lax.axis_index("row"), lax.axis_index("col")
    mine = features.shape[0] // block
    columns = block_cols[0, 0] - col * (mine * row_count)
    index = ((columns // mine) ^ row) * mine + columns % mine
    slot_ids = jnp.arange(slots, dtype=jnp.int32)
    rows = jnp.sum((pointers[None, 1:] <= slot_ids[:, None]).astype(jnp.int32), axis=1)
    owned = local_rows // col_count

    kinds = []
    for d, right, left, both in plan(col_count):
        if both:
            kinds.append((d, "both", right + left, jnp.where(col + d < col_count, col + d, col - d)))
        else:
            kinds.append((d, "right", right, col + d))
            kinds.append((d, "left", left, col - d))
    owners = jnp.clip(jnp.stack([k[3] for k in kinds] + [col]), 0, col_count - 1).astype(jnp.int32)

    width = features.shape[1]
    parts = [gather(features[:, at : at + LANES], row_count) for at in range(0, width, LANES)]
    outs = []
    for pieces in parts:
        messages, own = products(
            pointers[local_rows:], index, rows, owners, values, pieces, owned, local_rows
        )
        got = []
        relayed = {}
        for (d, side, pairs, _), message in zip(kinds, messages):
            sides = ("right", "left") if side == "both" else (side,)
            incoming = []
            for s in sides:
                for array in relayed.get((d + 1, s), []):
                    if not any(array is a for a in incoming):
                        incoming.append(array)
            fed = set()
            for s in sides:
                fed |= relayed.get((d + 1, s, "to"), set())
            if d >= 3:
                if incoming:
                    message = merge([message] + incoming, block, owned)
                hops = [(a, a + 1 if b > a else a - 1) for a, b in pairs]
                array = lax.ppermute(message, "col", hops)
                for s in sides:
                    relayed.setdefault((d, s), []).append(array)
                    relayed.setdefault((d, s, "to"), set()).update(
                        b for a, b in hops if (b > a) == (s == "right")
                    )
            else:
                plain = [pair for pair in pairs if pair[0] not in fed]
                late = [pair for pair in pairs if pair[0] in fed]
                if plain:
                    got.append(lax.ppermute(message, "col", plain))
                if late:
                    merged = merge([message] + incoming, block, owned)
                    got.append(lax.ppermute(merged, "col", late))
        outs.append(finish(own, got))
    return jnp.concatenate(outs, axis=1)


def solution(mesh):
    return jax.shard_map(
        local,
        mesh=mesh,
        in_specs=(
            P(("col", "row"), None),
            P("row", "col", None, None, None),
            P("row", "col", None),
            P("row", "col", None),
        ),
        out_specs=P(("row", "col"), None),
        check_vma=False,
    )
```

```python
import functools

import jax
import jax.numpy as jnp
from jax import lax
from jax.experimental import pallas as pl
from jax.experimental.pallas import tpu as pltpu
from jax.sharding import PartitionSpec as P


LANES = 128
UNROLL = 8
MIB = 1 << 20
CHUNKS = (4, 4, 2)
TOP = 32700.0
STEPS = 8.0
TINY = 2.0**-110


def code_of(peak):
    return jnp.ceil(jnp.log2(jnp.maximum(peak, TINY)) * STEPS)


def encode(y):
    code = code_of(jnp.max(jnp.abs(y), axis=0, keepdims=True))
    coded = jnp.round(y * (jnp.exp2(code * (-1.0 / STEPS)) * TOP))
    return coded.astype(jnp.int32).astype(jnp.int16), code


def scale_of(codes):
    return jnp.exp2(codes.astype(jnp.float32) * (1.0 / STEPS)) * (1.0 / TOP)


def rows_of(i, size):
    return pl.ds(pl.multiple_of(i * size, size), size)


def params(mib):
    return pltpu.CompilerParams(vmem_limit_bytes=mib * MIB)


def turn_kernel(block, sizes, x_ref, *out_refs):
    @pl.loop(0, out_refs[0].shape[0])
    def _(j):
        y = x_ref[rows_of(j, block), :].T
        at = 0
        for width, out_ref in zip(sizes, out_refs):
            out_ref[j] = y[at : at + width, :]
            at += width


def turn(features, block, place, sizes):
    rows = features.shape[0]
    mine, width = rows // block, sum(sizes)
    whole = lambda shape: pl.BlockSpec(shape, functools.partial(lambda n, i: (0,) * n, len(shape)))
    shapes = [(mine, size, block) for size in sizes]
    return pl.pallas_call(
        functools.partial(turn_kernel, block, sizes),
        out_shape=[jax.ShapeDtypeStruct(shape, features.dtype) for shape in shapes],
        grid=(1,),
        in_specs=[pl.BlockSpec((rows, width), lambda i: (0, place))],
        out_specs=[whole(shape) for shape in shapes],
        compiler_params=params(8),
        cost_estimate=pl.CostEstimate(flops=1 << 26, bytes_accessed=1 << 20, transcendentals=0),
    )(features)


def stage_kernel(
    owner_of, mine, pointer_ref, column_ref, values_ref, range_ref, index_ref, row_ref, store_ref, sem
):
    local_rows = pointer_ref.shape[0] - 1
    slots = column_ref.shape[0]
    count = pointer_ref[local_rows]
    steps = (count + UNROLL - 1) // UNROLL

    def copy(t):
        span = pl.ds(t * UNROLL, UNROLL)
        return pltpu.make_async_copy(values_ref.at[span], store_ref.at[span], sem.at[t])

    @pl.loop(0, steps)
    def _(t):
        copy(t).start()

    row, col = lax.axis_index("row"), lax.axis_index("col")
    group = mine * lax.axis_size("row")

    @pl.loop(0, slots)
    def _(s):
        column = column_ref[s] - col * group
        device = lax.div(column, mine)
        index_ref[s] = (device ^ row) * mine + column - device * mine
        row_ref[s] = local_rows

    @pl.loop(0, local_rows)
    def _(i):
        @pl.loop(pointer_ref[i], pointer_ref[i + 1])
        def _(s):
            row_ref[s] = i

    owned = local_rows // lax.axis_size("col")
    for m, owner in enumerate(owner_of(col)):
        first = jnp.clip(owner, 0, lax.axis_size("col") - 1) * owned
        range_ref[3 * m] = pointer_ref[first]
        range_ref[3 * m + 1] = pointer_ref[first + owned]
        range_ref[3 * m + 2] = first

    @pl.loop(0, steps)
    def _(t):
        copy(t).wait()


def stage(pointers, columns, values, owner_of, count, mine):
    smem = pl.BlockSpec(memory_space=pltpu.SMEM)
    slots = values.shape[0]
    return pl.pallas_call(
        functools.partial(stage_kernel, owner_of, mine),
        out_shape=[
            jax.ShapeDtypeStruct((3 * count,), jnp.int32),
            jax.ShapeDtypeStruct((slots,), jnp.int32),
            jax.ShapeDtypeStruct((slots,), jnp.int32),
            jax.ShapeDtypeStruct(values.shape, values.dtype),
        ],
        in_specs=[smem, smem, pl.BlockSpec(memory_space=pltpu.HBM)],
        out_specs=[smem] * 3 + [pl.BlockSpec(memory_space=pltpu.VMEM)],
        scratch_shapes=[pltpu.SemaphoreType.DMA((slots // UNROLL,))],
        compiler_params=params(8),
        cost_estimate=pl.CostEstimate(flops=1 << 26, bytes_accessed=1 << 22, transcendentals=0),
    )(pointers, columns, values)


def product_kernel(sizes, range_ref, index_ref, row_ref, store, *refs):
    pieces, start, messages, own, owned, mine, width = sizes
    piece_refs = refs[:pieces]
    out_refs = refs[pieces : pieces + messages + own]
    panel, scratch, codes = refs[pieces + messages + own :]

    for p in range(pieces):

        @pl.loop(0, mine)
        def _(j):
            panel[p * mine + j] = piece_refs[p][j]

    for m in range(messages + own):
        low, high, first_row = (range_ref[3 * (start + m) + n] for n in range(3))
        acc = scratch if m < messages else out_refs[m]

        @pl.loop(0, owned)
        def _(i):
            acc[i] = jnp.zeros((width, LANES), jnp.float32)

        @pl.loop(0, (high - low + UNROLL - 1) // UNROLL)
        def _(t):
            terms = []
            for u in range(UNROLL):
                s = low + t * UNROLL + u
                terms.append(
                    lax.dot_general(
                        panel[index_ref[s]],
                        store[s],
                        (((1,), (1,)), ((), ())),
                        preferred_element_type=jnp.float32,
                    )
                )
            for u in range(UNROLL):
                s = low + t * UNROLL + u
                acc[jnp.where(s < high, row_ref[s] - first_row, owned)] += terms[u]

        if m < messages:

            @pl.loop(0, owned)
            def _(i):
                y, code = encode(acc[i])
                out_refs[m][rows_of(i, width), :] = y
                codes[pl.ds(i, 1), :] = code

            tail = codes.shape[0]
            out_refs[m][owned * width : owned * width + tail, :] = (
                codes[...].astype(jnp.int32).astype(jnp.int16)
            )


def products(ranges, index, rows, store, pieces, owned, start, messages, own):
    slots, block = store.shape[:2]
    mine, width = pieces[0].shape[:2]
    tail = -(-owned // 16) * 16
    length = owned * width + tail
    smem = pl.BlockSpec(memory_space=pltpu.SMEM)
    whole = pl.BlockSpec(memory_space=pltpu.VMEM)
    flops = 2 * slots * block * block * width
    return pl.pallas_call(
        functools.partial(
            product_kernel, (len(pieces), start, messages, own, owned, mine, width)
        ),
        out_shape=[jax.ShapeDtypeStruct((length, block), jnp.int16)] * messages
        + [jax.ShapeDtypeStruct((owned + 1, width, block), jnp.float32)] * own,
        in_specs=[smem] * 3 + [whole] * (1 + len(pieces)),
        out_specs=[whole] * (messages + own),
        scratch_shapes=[
            pltpu.VMEM((len(pieces) * mine, width, block), store.dtype),
            pltpu.VMEM((owned + 1, width, block), jnp.float32),
            pltpu.VMEM((tail, block), jnp.float32),
        ],
        compiler_params=params(20),
        cost_estimate=pl.CostEstimate(flops=2 * flops, bytes_accessed=1 << 23, transcendentals=0),
    )(ranges, index, rows, store, *pieces)


def decoded(ref, codes, i, width):
    q = ref[rows_of(i, width), :]
    return q.astype(jnp.int32).astype(jnp.float32) * codes[pl.ds(i, 1), :]


def merge_kernel(width, owned, *refs):
    *in_refs, out_ref, codes, new = refs
    for n, ref in enumerate(in_refs):
        codes[n] = scale_of(ref[owned * width :, :].astype(jnp.int32))

    @pl.loop(0, owned)
    def _(i):
        total = sum(decoded(ref, codes.at[n], i, width) for n, ref in enumerate(in_refs))
        y, code = encode(total)
        out_ref[rows_of(i, width), :] = y
        new[pl.ds(i, 1), :] = code

    out_ref[owned * width :, :] = new[...].astype(jnp.int32).astype(jnp.int16)


def merge(terms, width, owned):
    length, block = terms[0].shape
    tail = length - owned * width
    whole = pl.BlockSpec(memory_space=pltpu.VMEM)
    return pl.pallas_call(
        functools.partial(merge_kernel, width, owned),
        out_shape=jax.ShapeDtypeStruct((length, block), jnp.int16),
        in_specs=[whole] * len(terms),
        out_specs=whole,
        scratch_shapes=[
            pltpu.VMEM((len(terms), tail, block), jnp.float32),
            pltpu.VMEM((tail, block), jnp.float32),
        ],
        compiler_params=params(6),
        cost_estimate=pl.CostEstimate(
            flops=1 << 28, bytes_accessed=3 * length * width * 2, transcendentals=0
        ),
    )(*terms)


def finish_kernel(owned, groups, *refs):
    out_ref, total = refs[-2:]
    block = total.shape[1]
    refs = refs[:-2]

    @pl.loop(0, owned)
    def _(i):
        at, offset = 0, 0
        for width, terms in groups:
            y = refs[at][i]
            for ref in refs[at + 1 : at + 1 + terms]:
                scale = scale_of(ref[owned * width :, :].astype(jnp.int32))
                here = lax.broadcasted_iota(jnp.int32, scale.shape, 0) == i
                row = jnp.sum(jnp.where(here, scale, 0.0), axis=0, keepdims=True)
                y = y + ref[rows_of(i, width), :].astype(jnp.int32).astype(jnp.float32) * row
            total[offset : offset + width, :] = y
            at, offset = at + 1 + terms, offset + width
        out_ref[rows_of(i, block), :] = total[...].T.astype(out_ref.dtype)


def finish(groups, owned_rows, place, spans, earlier):
    arrays, sizes = [], []
    for own, got in groups:
        arrays += [own, *got]
        sizes.append((own.shape[1], len(got)))
    owned, block = owned_rows, groups[0][0].shape[2]
    width = sum(size for size, _ in sizes)
    specs = [pl.BlockSpec(a.shape, functools.partial(lambda n, i: (0,) * n, a.ndim)) for a in arrays]
    aliases = {}
    if earlier is not None:
        aliases = {len(arrays): 0}
        arrays.append(earlier)
        specs.append(pl.BlockSpec(memory_space=pl.ANY))
    return pl.pallas_call(
        functools.partial(finish_kernel, owned, sizes),
        out_shape=jax.ShapeDtypeStruct((owned * block, width * spans), jnp.bfloat16),
        grid=(1,),
        in_specs=specs,
        out_specs=pl.BlockSpec((owned * block, width), lambda i: (0, place)),
        scratch_shapes=[pltpu.VMEM((width, block), jnp.float32)],
        input_output_aliases=aliases,
        compiler_params=params(16),
        cost_estimate=pl.CostEstimate(
            flops=1 << 28, bytes_accessed=1 << 22, transcendentals=0
        ),
    )(*arrays)


def gather(part, devices):
    pieces = []
    for p in range(0, devices, 2):
        near = part if p == 0 else lax.ppermute(part, "row", [(d, d ^ p) for d in range(devices)])
        pieces += [near, lax.ppermute(near, "row", [(d, d ^ 1) for d in range(devices)])]
    return pieces


def plan(count):
    out = []
    for d in range(count - 1, 0, -1):
        right = [(z, z + d) for z in range(count - d)]
        left = [(z, z - d) for z in range(d, count)]
        out.append((d, right, left, count - 1 - d < d - 1 or (d == 2 and count == 4)))
    return out


def reduce(kinds, messages, width, owned):
    got = []
    relayed = {}
    for (d, side, pairs), message in zip(kinds, messages):
        sides = ("right", "left") if side == "both" else (side,)
        incoming = []
        fed = set()
        for s in sides:
            for array in relayed.get((d + 1, s), []):
                if not any(array is a for a in incoming):
                    incoming.append(array)
            fed |= relayed.get((d + 1, s, "to"), set())
        if d >= 3:
            if incoming:
                message = merge([message] + incoming, width, owned)
            hops = [(a, a + 1 if b > a else a - 1) for a, b in pairs]
            array = lax.ppermute(message, "col", hops)
            for s in sides:
                relayed.setdefault((d, s), []).append(array)
                relayed.setdefault((d, s, "to"), set()).update(
                    b for a, b in hops if (b > a) == (s == "right")
                )
        else:
            plain = [pair for pair in pairs if pair[0] not in fed]
            late = [pair for pair in pairs if pair[0] in fed]
            if plain:
                got.append(lax.ppermute(message, "col", plain))
            if late:
                merged = merge([message] + incoming, width, owned)
                got.append(lax.ppermute(merged, "col", late))
    return got


def local(features, block_values, row_ptr, block_cols):
    values = block_values[0, 0]
    pointers = row_ptr[0, 0]
    block = values.shape[1]
    row_count, col_count = lax.axis_size("row"), lax.axis_size("col")
    mine = features.shape[0] // block
    total_width = features.shape[1]
    owned = (pointers.shape[0] - 1) // col_count

    kinds = []
    for d, right, left, both in plan(col_count):
        if both:
            kinds.append((d, "both", right + left))
        else:
            kinds.append((d, "right", right))
            kinds.append((d, "left", left))

    def owner_of(col):
        for d, side, _ in kinds:
            right = side == "right" if side != "both" else col + d < col_count
            yield jnp.where(right, col + d, col - d)
        yield col

    widths = [total_width // part for part in CHUNKS]
    turned, taken = [], []
    for width in widths:
        taken.append(width)
        if sum(taken) % LANES == 0:
            turned += turn(features, block, sum(widths[: len(turned)]) // LANES, taken)
            taken = []
    parts = [gather(piece, row_count) for piece in turned]
    ranges, index, rows, store = stage(
        pointers, block_cols[0, 0], values, owner_of, len(kinds) + 1, mine
    )
    groups, filled, out = [], 0, None
    for width, pieces in zip(widths, parts):
        lead = products(ranges, index, rows, store, pieces, owned, 0, 1, 0)
        *others, own = products(
            ranges, index, rows, store, pieces, owned, 1, len(kinds) - 1, 1
        )
        groups.append((own, reduce(kinds, [*lead, *others], width, owned)))
        filled += width
        if filled % LANES == 0:
            out = finish(groups, owned, filled // LANES - 1, total_width // LANES, out)
            groups = []
    return out


def solution(mesh):
    return jax.shard_map(
        local,
        mesh=mesh,
        in_specs=(
            P(("col", "row"), None),
            P("row", "col", None, None, None),
            P("row", "col", None),
            P("row", "col", None),
        ),
        out_specs=P(("row", "col"), None),
        check_vma=False,
    )
```

```python
import functools

import jax
import jax.numpy as jnp
from jax import lax
from jax.experimental import pallas as pl
from jax.experimental.pallas import tpu as pltpu
from jax.sharding import PartitionSpec as P


LANES = 128
UNROLL = 16
MIB = 1 << 20
CHUNKS = (8, 8)
TOP = 32700.0
STEPS = 8.0
TINY = 2.0**-110


def code_of(peak):
    return jnp.ceil(jnp.log2(jnp.maximum(peak, TINY)) * STEPS)


def encode(y):
    code = code_of(jnp.max(jnp.abs(y), axis=0, keepdims=True))
    coded = jnp.round(y * (jnp.exp2(code * (-1.0 / STEPS)) * TOP))
    return coded.astype(jnp.int32).astype(jnp.int16), code


def scale_of(codes):
    return jnp.exp2(codes.astype(jnp.float32) * (1.0 / STEPS)) * (1.0 / TOP)


def rows_of(i, size):
    return pl.ds(pl.multiple_of(i * size, size), size)


def params(mib):
    return pltpu.CompilerParams(vmem_limit_bytes=mib * MIB)


def turn_kernel(block, first, x_ref, out_ref):
    mine, width = out_ref.shape[:2]
    aligned, last = first // LANES * LANES, first + width
    end = -(-last // LANES) * LANES

    @pl.loop(0, mine, unroll=4)
    def _(j):
        y = x_ref[rows_of(j, block), aligned:end].T
        out_ref[j] = y[first - aligned : last - aligned, :]


def turn(features, block, first, width):
    mine = features.shape[0] // block
    whole = pl.BlockSpec(memory_space=pltpu.VMEM)
    return pl.pallas_call(
        functools.partial(turn_kernel, block, first),
        out_shape=jax.ShapeDtypeStruct((mine, width, block), features.dtype),
        in_specs=[whole],
        out_specs=whole,
        compiler_params=params(4),
        cost_estimate=pl.CostEstimate(flops=1 << 26, bytes_accessed=1 << 20, transcendentals=0),
    )(features)


def stage_kernel(
    owner_of, mine, pointer_ref, column_ref, values_ref, range_ref, index_ref, row_ref, store_ref
):
    local_rows = pointer_ref.shape[0] - 1
    slots = column_ref.shape[0]
    row, col = lax.axis_index("row"), lax.axis_index("col")
    group = mine * lax.axis_size("row")

    @pl.loop(0, slots, unroll=4)
    def _(s):
        column = column_ref[s] - col * group
        device = lax.div(column, mine)
        index_ref[s] = (device ^ row) * mine + column - device * mine
        row_ref[s] = local_rows

    @pl.loop(0, local_rows)
    def _(i):
        @pl.loop(pointer_ref[i], pointer_ref[i + 1])
        def _(s):
            row_ref[s] = i

    owned = local_rows // lax.axis_size("col")
    for m, owner in enumerate(owner_of(col)):
        first = jnp.clip(owner, 0, lax.axis_size("col") - 1) * owned
        sent = (owner >= 0) & (owner < lax.axis_size("col"))
        range_ref[3 * m] = jnp.where(sent, pointer_ref[first], 0)
        range_ref[3 * m + 1] = jnp.where(sent, pointer_ref[first + owned], 0)
        range_ref[3 * m + 2] = first
    range_ref[3 * m + 3] = pointer_ref[local_rows]

    @pl.loop(0, (pointer_ref[local_rows] + 3) // 4)
    def _(t):
        for u in range(4):
            store_ref[4 * t + u] = values_ref[4 * t + u].T


def stage(pointers, columns, values, owner_of, count, mine):
    smem = pl.BlockSpec(memory_space=pltpu.SMEM)
    whole = pl.BlockSpec(memory_space=pltpu.VMEM)
    slots = columns.shape[0]
    return pl.pallas_call(
        functools.partial(stage_kernel, owner_of, mine),
        out_shape=[
            jax.ShapeDtypeStruct((3 * count + 1,), jnp.int32),
            jax.ShapeDtypeStruct((slots,), jnp.int32),
            jax.ShapeDtypeStruct((slots,), jnp.int32),
            jax.ShapeDtypeStruct(values.shape, values.dtype),
        ],
        in_specs=[smem, smem, whole],
        out_specs=[smem] * 3 + [whole],
        compiler_params=params(4),
        cost_estimate=pl.CostEstimate(flops=1 << 26, bytes_accessed=1 << 12, transcendentals=0),
    )(pointers, columns, values)


def add_slots(low, high, spare, offset, index_ref, row_ref, store, panel, acc):
    @pl.loop(0, (high - low + UNROLL - 1) // UNROLL)
    def _(t):
        terms = []
        for u in range(UNROLL):
            s = low + t * UNROLL + u
            terms.append(
                jnp.dot(panel[index_ref[s]], store[s], preferred_element_type=jnp.float32)
            )
        for u in range(UNROLL):
            s = low + t * UNROLL + u
            acc[jnp.where(s < high, row_ref[s] - offset, spare)] += terms[u]


def write_message(acc, first, out_ref, codes, owned, width):
    @pl.loop(0, owned, unroll=4)
    def _(i):
        y, code = encode(acc[first + i])
        out_ref[rows_of(i, width), :] = y
        codes[pl.ds(i, 1), :] = code

    out_ref[owned * width :, :] = codes[...].astype(jnp.int32).astype(jnp.int16)


def clear(acc, count):
    @pl.loop(0, count, unroll=4)
    def _(i):
        acc[i] = jnp.zeros(acc.shape[1:], acc.dtype)


def head_kernel(owned, range_ref, index_ref, row_ref, store, *refs):
    *piece_refs, out_ref, panel, acc, codes = refs
    mine, width = piece_refs[0].shape[:2]

    for p, ref in enumerate(piece_refs):

        @pl.loop(0, mine, unroll=4)
        def _(j):
            panel[p * mine + j] = ref[j]

    clear(acc, owned)
    low, high, first = (range_ref[n] for n in range(3))
    add_slots(low, high, owned, first, index_ref, row_ref, store, panel, acc)
    write_message(acc, 0, out_ref, codes, owned, width)


def rest_kernel(owned, messages, local_rows, range_ref, index_ref, row_ref, store, panel, *refs):
    out_refs = refs[:messages]
    own_ref, acc, codes = refs[messages:]
    width = panel.shape[1]
    clear(acc, local_rows)
    low, high, total = range_ref[0], range_ref[1], range_ref[3 * messages + 6]
    add_slots(0, low, local_rows, 0, index_ref, row_ref, store, panel, acc)
    add_slots(high, total, local_rows, 0, index_ref, row_ref, store, panel, acc)
    for m, out_ref in enumerate(out_refs):
        write_message(acc, range_ref[3 * m + 5], out_ref, codes, owned, width)
    first = range_ref[3 * messages + 5]

    @pl.loop(0, owned, unroll=4)
    def _(i):
        own_ref[i] = acc[first + i]


def head(ranges, index, rows, store, pieces, owned):
    slots, block = store.shape[:2]
    mine, width = pieces[0].shape[:2]
    tail = -(-owned // 16) * 16
    smem = pl.BlockSpec(memory_space=pltpu.SMEM)
    whole = pl.BlockSpec(memory_space=pltpu.VMEM)
    flops = slots * block * block * width
    return pl.pallas_call(
        functools.partial(head_kernel, owned),
        out_shape=[
            jax.ShapeDtypeStruct((owned * width + tail, block), jnp.int16),
            jax.ShapeDtypeStruct((len(pieces) * mine, width, block), store.dtype),
        ],
        in_specs=[smem] * 3 + [whole] * (1 + len(pieces)),
        out_specs=[whole] * 2,
        scratch_shapes=[
            pltpu.VMEM((owned + 1, width, block), jnp.float32),
            pltpu.VMEM((tail, block), jnp.float32),
        ],
        compiler_params=params(10),
        cost_estimate=pl.CostEstimate(flops=flops, bytes_accessed=1 << 22, transcendentals=0),
    )(ranges, index, rows, store, *pieces)


def rest(ranges, index, rows, store, panel, owned, local_rows, messages):
    slots, block = store.shape[:2]
    width = panel.shape[1]
    tail = -(-owned // 16) * 16
    smem = pl.BlockSpec(memory_space=pltpu.SMEM)
    whole = pl.BlockSpec(memory_space=pltpu.VMEM)
    flops = 2 * slots * block * block * width
    return pl.pallas_call(
        functools.partial(rest_kernel, owned, messages, local_rows),
        out_shape=[jax.ShapeDtypeStruct((owned * width + tail, block), jnp.int16)] * messages
        + [jax.ShapeDtypeStruct((owned, width, block), jnp.float32)],
        in_specs=[smem] * 3 + [whole] * 2,
        out_specs=[whole] * (messages + 1),
        scratch_shapes=[
            pltpu.VMEM((local_rows + 1, width, block), jnp.float32),
            pltpu.VMEM((tail, block), jnp.float32),
        ],
        compiler_params=params(12),
        cost_estimate=pl.CostEstimate(flops=flops, bytes_accessed=1 << 22, transcendentals=0),
    )(ranges, index, rows, store, panel)


def decoded(ref, codes, i, width):
    q = ref[rows_of(i, width), :]
    return q.astype(jnp.int32).astype(jnp.float32) * codes[pl.ds(i, 1), :]


def merge_kernel(width, owned, *refs):
    *in_refs, out_ref, codes, new = refs
    for n, ref in enumerate(in_refs):
        codes[n] = scale_of(ref[owned * width :, :].astype(jnp.int32))

    @pl.loop(0, owned, unroll=4)
    def _(i):
        total = sum(decoded(ref, codes.at[n], i, width) for n, ref in enumerate(in_refs))
        y, code = encode(total)
        out_ref[rows_of(i, width), :] = y
        new[pl.ds(i, 1), :] = code

    out_ref[owned * width :, :] = new[...].astype(jnp.int32).astype(jnp.int16)


def merge(terms, width, owned):
    length, block = terms[0].shape
    tail = length - owned * width
    whole = pl.BlockSpec(memory_space=pltpu.VMEM)
    return pl.pallas_call(
        functools.partial(merge_kernel, width, owned),
        out_shape=jax.ShapeDtypeStruct((length, block), jnp.int16),
        in_specs=[whole] * len(terms),
        out_specs=whole,
        scratch_shapes=[
            pltpu.VMEM((len(terms), tail, block), jnp.float32),
            pltpu.VMEM((tail, block), jnp.float32),
        ],
        compiler_params=params(6),
        cost_estimate=pl.CostEstimate(
            flops=1 << 28, bytes_accessed=3 * length * width * 2, transcendentals=0
        ),
    )(*terms)


def finish_kernel(owned, parts, *refs):
    count = sum(1 + part[3] for part in parts)
    out_ref = refs[-2 - sum(part[3] for part in parts)]
    total, codes = refs[-1 - sum(part[3] for part in parts)], refs[-sum(part[3] for part in parts) :]
    in_refs = refs[:count]
    block = total.shape[2]

    at, n = 0, 0
    for width, _, _, terms in parts:
        for ref in in_refs[at + 1 : at + 1 + terms]:
            codes[n][...] = scale_of(ref[owned * width :, :].astype(jnp.int32))
            n += 1
        at += 1 + terms

    @pl.loop(0, owned // 2, unroll=2)
    def _(h):
        for k in range(2):
            i = 2 * h + k
            at, n, offset = 0, 0, 0
            for width, first, last, terms in parts:
                y = in_refs[at][i, first:last, :]
                for ref in in_refs[at + 1 : at + 1 + terms]:
                    rows = pl.ds(pl.multiple_of(i * width + first, 16), last - first)
                    y = y + ref[rows, :].astype(jnp.int32).astype(jnp.float32) * codes[n][pl.ds(i, 1), :]
                    n += 1
                total[k, offset : offset + last - first, :] = y
                at, offset = at + 1 + terms, offset + last - first
            out_ref[rows_of(i, block), :] = total[k].T.astype(out_ref.dtype)


def finish(parts, owned, place, spans, earlier):
    arrays, sizes = [], []
    for own, got, first, last in parts:
        arrays += [own, *got]
        sizes.append((own.shape[1], first, last, len(got)))
    block = own.shape[2]
    tail = got[0].shape[0] - owned * own.shape[1]
    specs = [pl.BlockSpec(a.shape, functools.partial(lambda n, i: (0,) * n, a.ndim)) for a in arrays]
    aliases = {}
    if earlier is not None:
        aliases = {len(arrays): 0}
        arrays.append(earlier)
        specs.append(pl.BlockSpec(memory_space=pl.ANY))
    return pl.pallas_call(
        functools.partial(finish_kernel, owned, sizes),
        out_shape=jax.ShapeDtypeStruct((owned * block, LANES * spans), jnp.bfloat16),
        grid=(1,),
        in_specs=specs,
        out_specs=pl.BlockSpec((owned * block, LANES), lambda i: (0, place)),
        scratch_shapes=[pltpu.VMEM((2, LANES, block), jnp.float32)]
        + [pltpu.VMEM((tail, block), jnp.float32)] * sum(size[3] for size in sizes),
        input_output_aliases=aliases,
        compiler_params=params(12),
        cost_estimate=pl.CostEstimate(
            flops=1 << 28, bytes_accessed=1 << 22, transcendentals=0
        ),
    )(*arrays)


def gather(part, devices):
    pieces = []
    for p in range(0, devices, 2):
        near = part if p == 0 else lax.ppermute(part, "row", [(d, d ^ p) for d in range(devices)])
        pieces += [near, lax.ppermute(near, "row", [(d, d ^ 1) for d in range(devices)])]
    return pieces


def plan(count):
    out = []
    for d in range(count - 1, 0, -1):
        right = [(z, z + d) for z in range(count - d)]
        left = [(z, z - d) for z in range(d, count)]
        out.append((d, right, left, count - 1 - d < d - 1 or (d == 2 and count == 4)))
    return out


def reduce(kinds, messages, width, owned):
    got = []
    relayed = {}
    for (d, side, pairs), message in zip(kinds, messages):
        sides = ("right", "left") if side == "both" else (side,)
        incoming = []
        for s in sides:
            for array in relayed.get((d + 1, s), []):
                if not any(array is a for a in incoming):
                    incoming.append(array)
        if d >= 3:
            if incoming:
                message = merge([message] + incoming, width, owned)
            hops = [(a, a + 1 if b > a else a - 1) for a, b in pairs]
            array = lax.ppermute(message, "col", hops)
            for s in sides:
                relayed.setdefault((d, s), []).append(array)
        elif incoming:
            merged = merge([message] + incoming, width, owned)
            got.append(lax.ppermute(merged, "col", pairs))
        else:
            got.append(lax.ppermute(message, "col", pairs))
    return got


def local(features, block_values, row_ptr, block_cols):
    values = block_values[0, 0]
    pointers = row_ptr[0, 0]
    block = values.shape[1]
    row_count, col_count = lax.axis_size("row"), lax.axis_size("col")
    mine = features.shape[0] // block
    total_width = features.shape[1]
    owned = (pointers.shape[0] - 1) // col_count

    kinds = []
    for d, right, left, both in plan(col_count):
        if both:
            kinds.append((d, "both", right + left))
        else:
            kinds.append((d, "right", right))
            kinds.append((d, "left", left))

    def owner_of(col):
        for d, side, _ in kinds:
            right = side == "right" if side != "both" else col + d < col_count
            yield jnp.where(right, col + d, col - d)
        yield col

    starts = [total_width * sum(CHUNKS[:n]) // sum(CHUNKS) for n in range(len(CHUNKS) + 1)]
    parts = []
    for first, last in zip(starts, starts[1:]):
        piece = turn(features, block, first, last - first)
        parts.append(gather(piece, row_count))
    ranges, index, rows, store = stage(
        pointers, block_cols[0, 0], values, owner_of, len(kinds) + 1, mine
    )
    sums, written, out = [], 0, None
    for chunk, pieces in enumerate(parts):
        lead, panel = head(ranges, index, rows, store, pieces, owned)
        *others, own = rest(
            ranges, index, rows, store, panel, owned, pointers.shape[0] - 1, len(kinds) - 1
        )
        got = reduce(kinds, [lead, *others], own.shape[1], owned)
        sums.append((own, got))
        while written + LANES <= starts[chunk + 1]:
            taken = [
                (*sums[n], max(written - first, 0), min(written + LANES, last) - first)
                for n, (first, last) in enumerate(zip(starts, starts[1:]))
                if first < written + LANES and last > written
            ]
            out = finish(taken, owned, written // LANES, total_width // LANES, out)
            written += LANES
    return out


def solution(mesh):
    return jax.shard_map(
        local,
        mesh=mesh,
        in_specs=(
            P(("col", "row"), None),
            P("row", "col", None, None, None),
            P("row", "col", None),
            P("row", "col", None),
        ),
        out_specs=P(("row", "col"), None),
        check_vma=False,
    )
```

```python
import functools

import jax
import jax.numpy as jnp
from jax import lax
from jax.experimental import pallas as pl
from jax.experimental.pallas import tpu as pltpu
from jax.sharding import PartitionSpec as P


LANES = 128
UNROLL = 16
MIB = 1 << 20
CHUNKS = (4, 6, 6)
TOP = 32700.0
STEPS = 8.0
TINY = 2.0**-110


def code_of(peak):
    return jnp.ceil(jnp.log2(jnp.maximum(peak, TINY)) * STEPS)


def encode(y):
    code = code_of(jnp.max(jnp.abs(y), axis=0, keepdims=True))
    coded = jnp.round(y * (jnp.exp2(code * (-1.0 / STEPS)) * TOP))
    return coded.astype(jnp.int32).astype(jnp.int16), code


def scale_of(codes):
    return jnp.exp2(codes.astype(jnp.float32) * (1.0 / STEPS)) * (1.0 / TOP)


def rows_of(i, size):
    return pl.ds(pl.multiple_of(i * size, size), size)


def params(mib):
    return pltpu.CompilerParams(vmem_limit_bytes=mib * MIB)


def turn_kernel(block, first, x_ref, out_ref):
    mine, width = out_ref.shape[:2]
    aligned, last = first // LANES * LANES, first + width
    end = -(-last // LANES) * LANES

    @pl.loop(0, mine, unroll=4)
    def _(j):
        y = x_ref[rows_of(j, block), aligned:end].T
        out_ref[j] = y[first - aligned : last - aligned, :]


def turn(features, block, first, width):
    mine = features.shape[0] // block
    whole = pl.BlockSpec(memory_space=pltpu.VMEM)
    return pl.pallas_call(
        functools.partial(turn_kernel, block, first),
        out_shape=jax.ShapeDtypeStruct((mine, width, block), features.dtype),
        in_specs=[whole],
        out_specs=whole,
        compiler_params=params(4),
        cost_estimate=pl.CostEstimate(flops=1 << 26, bytes_accessed=1 << 20, transcendentals=0),
    )(features)


def stage_kernel(
    owner_of, mine, pointer_ref, column_ref, values_ref, range_ref, index_ref, row_ref, store_ref
):
    local_rows = pointer_ref.shape[0] - 1
    slots = column_ref.shape[0]
    row, col = lax.axis_index("row"), lax.axis_index("col")
    group = mine * lax.axis_size("row")

    @pl.loop(0, slots, unroll=4)
    def _(s):
        column = column_ref[s] - col * group
        device = lax.div(column, mine)
        index_ref[s] = (device ^ row) * mine + column - device * mine
        row_ref[s] = local_rows

    @pl.loop(0, local_rows)
    def _(i):
        @pl.loop(pointer_ref[i], pointer_ref[i + 1])
        def _(s):
            row_ref[s] = i

    owned = local_rows // lax.axis_size("col")
    for m, owner in enumerate(owner_of(col)):
        first = jnp.clip(owner, 0, lax.axis_size("col") - 1) * owned
        sent = (owner >= 0) & (owner < lax.axis_size("col"))
        range_ref[3 * m] = jnp.where(sent, pointer_ref[first], 0)
        range_ref[3 * m + 1] = jnp.where(sent, pointer_ref[first + owned], 0)
        range_ref[3 * m + 2] = first
    range_ref[3 * m + 3] = pointer_ref[local_rows]

    @pl.loop(0, (pointer_ref[local_rows] + 3) // 4)
    def _(t):
        for u in range(4):
            store_ref[4 * t + u] = values_ref[4 * t + u].T


def stage(pointers, columns, values, owner_of, count, mine):
    smem = pl.BlockSpec(memory_space=pltpu.SMEM)
    whole = pl.BlockSpec(memory_space=pltpu.VMEM)
    slots = columns.shape[0]
    return pl.pallas_call(
        functools.partial(stage_kernel, owner_of, mine),
        out_shape=[
            jax.ShapeDtypeStruct((3 * count + 1,), jnp.int32),
            jax.ShapeDtypeStruct((slots,), jnp.int32),
            jax.ShapeDtypeStruct((slots,), jnp.int32),
            jax.ShapeDtypeStruct(values.shape, values.dtype),
        ],
        in_specs=[smem, smem, whole],
        out_specs=[smem] * 3 + [whole],
        compiler_params=params(4),
        cost_estimate=pl.CostEstimate(flops=1 << 26, bytes_accessed=1 << 12, transcendentals=0),
    )(pointers, columns, values)


def add_slots(low, high, spare, offset, index_ref, row_ref, store, panel, acc):
    @pl.loop(0, (high - low + UNROLL - 1) // UNROLL)
    def _(t):
        terms = []
        for u in range(UNROLL):
            s = low + t * UNROLL + u
            terms.append(
                jnp.dot(panel[index_ref[s]], store[s], preferred_element_type=jnp.float32)
            )
        for u in range(UNROLL):
            s = low + t * UNROLL + u
            acc[jnp.where(s < high, row_ref[s] - offset, spare)] += terms[u]


def write_message(acc, first, out_ref, codes, owned, width):
    @pl.loop(0, owned, unroll=4)
    def _(i):
        y, code = encode(acc[first + i])
        out_ref[rows_of(i, width), :] = y
        codes[pl.ds(i, 1), :] = code

    out_ref[owned * width :, :] = codes[...].astype(jnp.int32).astype(jnp.int16)


def clear(acc, count):
    @pl.loop(0, count, unroll=4)
    def _(i):
        acc[i] = jnp.zeros(acc.shape[1:], acc.dtype)


def head_kernel(owned, range_ref, index_ref, row_ref, store, *refs):
    *piece_refs, out_ref, panel, acc, codes = refs
    mine, width = piece_refs[0].shape[:2]

    for p, ref in enumerate(piece_refs):

        @pl.loop(0, mine, unroll=4)
        def _(j):
            panel[p * mine + j] = ref[j]

    clear(acc, owned)
    low, high, first = (range_ref[n] for n in range(3))
    add_slots(low, high, owned, first, index_ref, row_ref, store, panel, acc)
    write_message(acc, 0, out_ref, codes, owned, width)


def rest_kernel(owned, messages, local_rows, range_ref, index_ref, row_ref, store, panel, *refs):
    out_refs = refs[:messages]
    own_ref, acc, codes = refs[messages:]
    width = panel.shape[1]
    clear(acc, local_rows)
    low, high, total = range_ref[0], range_ref[1], range_ref[3 * messages + 6]
    add_slots(0, low, local_rows, 0, index_ref, row_ref, store, panel, acc)
    add_slots(high, total, local_rows, 0, index_ref, row_ref, store, panel, acc)
    for m, out_ref in enumerate(out_refs):
        write_message(acc, range_ref[3 * m + 5], out_ref, codes, owned, width)
    first = range_ref[3 * messages + 5]

    @pl.loop(0, owned, unroll=4)
    def _(i):
        own_ref[i] = acc[first + i]


def head(ranges, index, rows, store, pieces, owned):
    slots, block = store.shape[:2]
    mine, width = pieces[0].shape[:2]
    tail = -(-owned // 16) * 16
    smem = pl.BlockSpec(memory_space=pltpu.SMEM)
    whole = pl.BlockSpec(memory_space=pltpu.VMEM)
    flops = slots * block * block * width
    return pl.pallas_call(
        functools.partial(head_kernel, owned),
        out_shape=[
            jax.ShapeDtypeStruct((owned * width + tail, block), jnp.int16),
            jax.ShapeDtypeStruct((len(pieces) * mine, width, block), store.dtype),
        ],
        in_specs=[smem] * 3 + [whole] * (1 + len(pieces)),
        out_specs=[whole] * 2,
        scratch_shapes=[
            pltpu.VMEM((owned + 1, width, block), jnp.float32),
            pltpu.VMEM((tail, block), jnp.float32),
        ],
        compiler_params=params(10),
        cost_estimate=pl.CostEstimate(flops=flops, bytes_accessed=1 << 22, transcendentals=0),
    )(ranges, index, rows, store, *pieces)


def rest(ranges, index, rows, store, panel, owned, local_rows, messages):
    slots, block = store.shape[:2]
    width = panel.shape[1]
    tail = -(-owned // 16) * 16
    smem = pl.BlockSpec(memory_space=pltpu.SMEM)
    whole = pl.BlockSpec(memory_space=pltpu.VMEM)
    flops = 2 * slots * block * block * width
    return pl.pallas_call(
        functools.partial(rest_kernel, owned, messages, local_rows),
        out_shape=[jax.ShapeDtypeStruct((owned * width + tail, block), jnp.int16)] * messages
        + [jax.ShapeDtypeStruct((owned, width, block), jnp.float32)],
        in_specs=[smem] * 3 + [whole] * 2,
        out_specs=[whole] * (messages + 1),
        scratch_shapes=[
            pltpu.VMEM((local_rows + 1, width, block), jnp.float32),
            pltpu.VMEM((tail, block), jnp.float32),
        ],
        compiler_params=params(12),
        cost_estimate=pl.CostEstimate(flops=flops, bytes_accessed=1 << 22, transcendentals=0),
    )(ranges, index, rows, store, panel)


def decoded(ref, codes, i, width):
    q = ref[rows_of(i, width), :]
    return q.astype(jnp.int32).astype(jnp.float32) * codes[pl.ds(i, 1), :]


def merge_kernel(width, owned, *refs):
    *in_refs, out_ref, codes, new = refs
    for n, ref in enumerate(in_refs):
        codes[n] = scale_of(ref[owned * width :, :].astype(jnp.int32))

    @pl.loop(0, owned, unroll=4)
    def _(i):
        total = sum(decoded(ref, codes.at[n], i, width) for n, ref in enumerate(in_refs))
        y, code = encode(total)
        out_ref[rows_of(i, width), :] = y
        new[pl.ds(i, 1), :] = code

    out_ref[owned * width :, :] = new[...].astype(jnp.int32).astype(jnp.int16)


def merge(terms, width, owned):
    length, block = terms[0].shape
    tail = length - owned * width
    whole = pl.BlockSpec(memory_space=pltpu.VMEM)
    return pl.pallas_call(
        functools.partial(merge_kernel, width, owned),
        out_shape=jax.ShapeDtypeStruct((length, block), jnp.int16),
        in_specs=[whole] * len(terms),
        out_specs=whole,
        scratch_shapes=[
            pltpu.VMEM((len(terms), tail, block), jnp.float32),
            pltpu.VMEM((tail, block), jnp.float32),
        ],
        compiler_params=params(6),
        cost_estimate=pl.CostEstimate(
            flops=1 << 28, bytes_accessed=3 * length * width * 2, transcendentals=0
        ),
    )(*terms)


def finish_kernel(owned, parts, *refs):
    count = sum(1 + part[3] for part in parts)
    out_ref = refs[-2 - sum(part[3] for part in parts)]
    total, codes = refs[-1 - sum(part[3] for part in parts)], refs[-sum(part[3] for part in parts) :]
    in_refs = refs[:count]
    block = total.shape[2]

    at, n = 0, 0
    for width, _, _, terms in parts:
        for ref in in_refs[at + 1 : at + 1 + terms]:
            codes[n][...] = scale_of(ref[owned * width :, :].astype(jnp.int32))
            n += 1
        at += 1 + terms

    @pl.loop(0, owned // 2, unroll=2)
    def _(h):
        for k in range(2):
            i = 2 * h + k
            at, n, offset = 0, 0, 0
            for width, first, last, terms in parts:
                y = in_refs[at][i, first:last, :]
                for ref in in_refs[at + 1 : at + 1 + terms]:
                    rows = pl.ds(pl.multiple_of(i * width + first, 16), last - first)
                    y = y + ref[rows, :].astype(jnp.int32).astype(jnp.float32) * codes[n][pl.ds(i, 1), :]
                    n += 1
                total[k, offset : offset + last - first, :] = y
                at, offset = at + 1 + terms, offset + last - first
            out_ref[rows_of(i, block), :] = total[k].T.astype(out_ref.dtype)


def finish(parts, owned, place, spans, earlier):
    arrays, sizes = [], []
    for own, got, first, last in parts:
        arrays += [own, *got]
        sizes.append((own.shape[1], first, last, len(got)))
    block = own.shape[2]
    tail = got[0].shape[0] - owned * own.shape[1]
    specs = [pl.BlockSpec(a.shape, functools.partial(lambda n, i: (0,) * n, a.ndim)) for a in arrays]
    aliases = {}
    if earlier is not None:
        aliases = {len(arrays): 0}
        arrays.append(earlier)
        specs.append(pl.BlockSpec(memory_space=pl.ANY))
    return pl.pallas_call(
        functools.partial(finish_kernel, owned, sizes),
        out_shape=jax.ShapeDtypeStruct((owned * block, LANES * spans), jnp.bfloat16),
        grid=(1,),
        in_specs=specs,
        out_specs=pl.BlockSpec((owned * block, LANES), lambda i: (0, place)),
        scratch_shapes=[pltpu.VMEM((2, LANES, block), jnp.float32)]
        + [pltpu.VMEM((tail, block), jnp.float32)] * sum(size[3] for size in sizes),
        input_output_aliases=aliases,
        compiler_params=params(12),
        cost_estimate=pl.CostEstimate(
            flops=1 << 28, bytes_accessed=1 << 22, transcendentals=0
        ),
    )(*arrays)


def gather(part, devices):
    pieces = []
    for p in range(0, devices, 2):
        near = part if p == 0 else lax.ppermute(part, "row", [(d, d ^ p) for d in range(devices)])
        pieces += [near, lax.ppermute(near, "row", [(d, d ^ 1) for d in range(devices)])]
    return pieces


def plan(count):
    out = []
    for d in range(count - 1, 1, -1):
        right = [(z, z + d) for z in range(count - d)]
        left = [(z, z - d) for z in range(d, count)]
        hop = [(a, a + 1 if b > a else a - 1) for a, b in right + left]
        ends = [b for _, b in (hop if d > 2 else right + left)]
        if len(set(ends)) == len(ends) and count <= 2 * d:
            out.append(("both", d, right + left, lambda z, d=d: jnp.where(z + d < count, z + d, z - d)))
        else:
            out.append(("right", d, right, lambda z, d=d: z + d))
            out.append(("left", d, left, lambda z, d=d: z - d))
    outer = [(z, z ^ 1) for z in range(count) if z ^ 1 < count]
    middle = [(z, z + 1) for z in range(1, count - 1, 2)]
    out.append(("outer", 1, outer, lambda z: z ^ 1))
    if middle:
        middle += [(b, a) for a, b in middle]
        out.append(("middle", 1, middle, lambda z: z + 2 * (z & 1) - 1))
    return out


def shared(kinds):
    return kinds[-1][0] == "middle" and not {a for a, _ in kinds[0][2]} & {a for a, _ in kinds[-1][2]}


def reduce(kinds, messages, width, owned):
    got = []
    relayed = {}
    if shared(kinds):
        got.append(lax.ppermute(messages[0], "col", kinds[-1][2]))
    for (name, d, pairs, _), message in zip(kinds, messages):
        if d == 1:
            got.append(lax.ppermute(message, "col", pairs))
            continue
        sides = ("right", "left") if name == "both" else (name,)
        incoming = []
        for side in sides:
            for array in relayed.get((d + 1, side), []):
                if not any(array is a for a in incoming):
                    incoming.append(array)
        if incoming:
            message = merge([message] + incoming, width, owned)
        if d >= 3:
            hops = [(a, a + 1 if b > a else a - 1) for a, b in pairs]
            array = lax.ppermute(message, "col", hops)
            for side in sides:
                relayed.setdefault((d, side), []).append(array)
        else:
            got.append(lax.ppermute(message, "col", pairs))
    return got


def local(features, block_values, row_ptr, block_cols):
    values = block_values[0, 0]
    pointers = row_ptr[0, 0]
    block = values.shape[1]
    row_count, col_count = lax.axis_size("row"), lax.axis_size("col")
    mine = features.shape[0] // block
    total_width = features.shape[1]
    owned = (pointers.shape[0] - 1) // col_count

    kinds = plan(col_count)
    count = len(kinds) - shared(kinds)

    def owner_of(col):
        for n, (_, _, pairs, owner) in enumerate(kinds[:count]):
            there = owner(col)
            if n == 0 and shared(kinds):
                first = sum((col == a).astype(jnp.int32) for a, _ in pairs)
                there = jnp.where(first > 0, there, kinds[-1][3](col))
            yield there
        yield col

    starts = [total_width * sum(CHUNKS[:n]) // sum(CHUNKS) for n in range(len(CHUNKS) + 1)]
    parts = []
    for first, last in zip(starts, starts[1:]):
        piece = turn(features, block, first, last - first)
        parts.append(gather(piece, row_count))
    ranges, index, rows, store = stage(
        pointers, block_cols[0, 0], values, owner_of, count + 1, mine
    )
    sums, written, out = [], 0, None
    for chunk, pieces in enumerate(parts):
        lead, panel = head(ranges, index, rows, store, pieces, owned)
        *others, own = rest(
            ranges, index, rows, store, panel, owned, pointers.shape[0] - 1, count - 1
        )
        got = reduce(kinds, [lead, *others], own.shape[1], owned)
        sums.append((own, got))
        while written + LANES <= starts[chunk + 1]:
            taken = [
                (*sums[n], max(written - first, 0), min(written + LANES, last) - first)
                for n, (first, last) in enumerate(zip(starts, starts[1:]))
                if first < written + LANES and last > written
            ]
            out = finish(taken, owned, written // LANES, total_width // LANES, out)
            written += LANES
    return out


def solution(mesh):
    return jax.shard_map(
        local,
        mesh=mesh,
        in_specs=(
            P(("col", "row"), None),
            P("row", "col", None, None, None),
            P("row", "col", None),
            P("row", "col", None),
        ),
        out_specs=P(("row", "col"), None),
        check_vma=False,
    )
```

```python
import functools

import jax
import jax.numpy as jnp
from jax import lax
from jax.experimental import pallas as pl
from jax.experimental.pallas import tpu as pltpu
from jax.sharding import PartitionSpec as P


LANES = 128
UNROLL = 16
MIB = 1 << 20
STAGE_MIB = 46
DIRECT_CHUNKS = 1
CHUNKS = (3, 5, 8)
TOP = 32700.0
STEPS = 8.0
TINY = 2.0**-110


def code_of(peak):
    return jnp.ceil(jnp.log2(jnp.maximum(peak, TINY)) * STEPS)


def encode(y):
    code = code_of(jnp.max(jnp.abs(y), axis=0, keepdims=True))
    coded = jnp.round(y * (jnp.exp2(code * (-1.0 / STEPS)) * TOP))
    return coded.astype(jnp.int32).astype(jnp.int16), code


def scale_of(codes):
    return jnp.exp2(codes.astype(jnp.float32) * (1.0 / STEPS)) * (1.0 / TOP)


def rows_of(i, size):
    return pl.ds(pl.multiple_of(i * size, size), size)


def params(mib):
    return pltpu.CompilerParams(vmem_limit_bytes=mib * MIB)


def turn_kernel(block, first, x_ref, out_ref):
    mine, width = out_ref.shape[:2]
    aligned, last = first // LANES * LANES, first + width
    end = -(-last // LANES) * LANES

    @pl.loop(0, mine, unroll=4)
    def _(j):
        y = x_ref[rows_of(j, block), aligned:end].T
        out_ref[j] = y[first - aligned : last - aligned, :]


def turn(features, block, first, width):
    mine = features.shape[0] // block
    whole = pl.BlockSpec(memory_space=pltpu.VMEM)
    return pl.pallas_call(
        functools.partial(turn_kernel, block, first),
        out_shape=jax.ShapeDtypeStruct((mine, width, block), features.dtype),
        in_specs=[whole],
        out_specs=whole,
        compiler_params=params(4),
        cost_estimate=pl.CostEstimate(flops=1 << 26, bytes_accessed=1 << 20, transcendentals=0),
    )(features)


def stage_kernel(
    owner_of, mine, pointer_ref, column_ref, values_ref, range_ref, index_ref, row_ref, store_ref, sem
):
    local_rows = pointer_ref.shape[0] - 1
    slots = column_ref.shape[0]
    row, col = lax.axis_index("row"), lax.axis_index("col")
    group = mine * lax.axis_size("row")
    total = pointer_ref[local_rows]
    steps = (total + UNROLL - 1) // UNROLL

    def copy(t):
        span = pl.ds(t * UNROLL, UNROLL)
        return pltpu.make_async_copy(values_ref.at[span], store_ref.at[span], sem.at[t])

    @pl.loop(0, steps)
    def _(t):
        copy(t).start()

    @pl.loop(0, jnp.minimum(slots // UNROLL, steps + 1))
    def _(t):
        for u in range(UNROLL):
            column = column_ref[t * UNROLL + u] - col * group
            device = lax.div(column, mine)
            index_ref[t * UNROLL + u] = (device ^ row) * mine + column - device * mine

    @pl.loop(0, local_rows)
    def _(i):
        @pl.loop(pointer_ref[i], pointer_ref[i + 1])
        def _(s):
            row_ref[s] = i

    owned = local_rows // lax.axis_size("col")
    for m, owner in enumerate(owner_of(col)):
        first = jnp.clip(owner, 0, lax.axis_size("col") - 1) * owned
        sent = (owner >= 0) & (owner < lax.axis_size("col"))
        range_ref[3 * m] = jnp.where(sent, pointer_ref[first], 0)
        range_ref[3 * m + 1] = jnp.where(sent, pointer_ref[first + owned], 0)
        range_ref[3 * m + 2] = first
    range_ref[3 * m + 3] = total

    @pl.loop(0, steps)
    def _(t):
        copy(t).wait()


def stage(pointers, columns, values, owner_of, count, mine):
    smem = pl.BlockSpec(memory_space=pltpu.SMEM)
    whole = pl.BlockSpec(memory_space=pltpu.VMEM)
    slots = values.shape[0]
    return pl.pallas_call(
        functools.partial(stage_kernel, owner_of, mine),
        out_shape=[
            jax.ShapeDtypeStruct((3 * count + 1,), jnp.int32),
            jax.ShapeDtypeStruct((slots,), jnp.int32),
            jax.ShapeDtypeStruct((slots,), jnp.int32),
            jax.ShapeDtypeStruct(values.shape, values.dtype),
        ],
        in_specs=[smem, smem, pl.BlockSpec(memory_space=pltpu.HBM)],
        out_specs=[smem] * 3 + [whole],
        scratch_shapes=[pltpu.SemaphoreType.DMA((-(-slots // UNROLL),))],
        compiler_params=params(STAGE_MIB),
        cost_estimate=pl.CostEstimate(flops=1 << 26, bytes_accessed=1 << 22, transcendentals=0),
    )(pointers, columns, values)


def add_slots(low, high, spare, offset, index_ref, row_ref, store, panel, acc):
    @pl.loop(0, (high - low + UNROLL - 1) // UNROLL)
    def _(t):
        terms = []
        for u in range(UNROLL):
            s = low + t * UNROLL + u
            terms.append(
                lax.dot_general(
                    panel[index_ref[s]],
                    store[s],
                    (((1,), (1,)), ((), ())),
                    preferred_element_type=jnp.float32,
                )
            )
        for u in range(UNROLL):
            s = low + t * UNROLL + u
            acc[jnp.where(s < high, row_ref[s] - offset, spare)] += terms[u]


def write_message(acc, first, out_ref, codes, owned, width):
    @pl.loop(0, owned, unroll=4)
    def _(i):
        y, code = encode(acc[first + i])
        out_ref[rows_of(i, width), :] = y
        codes[pl.ds(i, 1), :] = code

    out_ref[owned * width :, :] = codes[...].astype(jnp.int32).astype(jnp.int16)


def clear(acc, count):
    @pl.loop(0, count, unroll=4)
    def _(i):
        acc[i] = jnp.zeros(acc.shape[1:], acc.dtype)


def head_kernel(owned, range_ref, index_ref, row_ref, store, *refs):
    *piece_refs, out_ref, panel, acc, codes = refs
    mine, width = piece_refs[0].shape[:2]

    for p, ref in enumerate(piece_refs):

        @pl.loop(0, mine, unroll=4)
        def _(j):
            panel[p * mine + j] = ref[j]

    clear(acc, owned)
    low, high, first = (range_ref[n] for n in range(3))
    add_slots(low, high, owned, first, index_ref, row_ref, store, panel, acc)
    write_message(acc, 0, out_ref, codes, owned, width)


def rest_kernel(owned, messages, local_rows, range_ref, index_ref, row_ref, store, panel, *refs):
    out_refs = refs[:messages]
    own_ref, acc, codes = refs[messages:]
    width = panel.shape[1]
    clear(acc, local_rows)
    low, high, total = range_ref[0], range_ref[1], range_ref[3 * messages + 6]
    add_slots(0, low, local_rows, 0, index_ref, row_ref, store, panel, acc)
    add_slots(high, total, local_rows, 0, index_ref, row_ref, store, panel, acc)
    for m, out_ref in enumerate(out_refs):
        write_message(acc, range_ref[3 * m + 5], out_ref, codes, owned, width)
    first = range_ref[3 * messages + 5]

    @pl.loop(0, owned, unroll=4)
    def _(i):
        own_ref[i] = acc[first + i]


def head(ranges, index, rows, store, pieces, owned):
    slots, block = store.shape[:2]
    mine, width = pieces[0].shape[:2]
    tail = -(-owned // 16) * 16
    smem = pl.BlockSpec(memory_space=pltpu.SMEM)
    whole = pl.BlockSpec(memory_space=pltpu.VMEM)
    flops = slots * block * block * width
    return pl.pallas_call(
        functools.partial(head_kernel, owned),
        out_shape=[
            jax.ShapeDtypeStruct((owned * width + tail, block), jnp.int16),
            jax.ShapeDtypeStruct((len(pieces) * mine, width, block), store.dtype),
        ],
        in_specs=[smem] * 3 + [whole] * (1 + len(pieces)),
        out_specs=[whole] * 2,
        scratch_shapes=[
            pltpu.VMEM((owned + 1, width, block), jnp.float32),
            pltpu.VMEM((tail, block), jnp.float32),
        ],
        compiler_params=params(10),
        cost_estimate=pl.CostEstimate(flops=flops, bytes_accessed=1 << 22, transcendentals=0),
    )(ranges, index, rows, store, *pieces)


def rest(ranges, index, rows, store, panel, owned, local_rows, messages):
    slots, block = store.shape[:2]
    width = panel.shape[1]
    tail = -(-owned // 16) * 16
    smem = pl.BlockSpec(memory_space=pltpu.SMEM)
    whole = pl.BlockSpec(memory_space=pltpu.VMEM)
    flops = 2 * slots * block * block * width
    return pl.pallas_call(
        functools.partial(rest_kernel, owned, messages, local_rows),
        out_shape=[jax.ShapeDtypeStruct((owned * width + tail, block), jnp.int16)] * messages
        + [jax.ShapeDtypeStruct((owned, width, block), jnp.float32)],
        in_specs=[smem] * 3 + [whole] * 2,
        out_specs=[whole] * (messages + 1),
        scratch_shapes=[
            pltpu.VMEM((local_rows + 1, width, block), jnp.float32),
            pltpu.VMEM((tail, block), jnp.float32),
        ],
        compiler_params=params(12),
        cost_estimate=pl.CostEstimate(flops=flops, bytes_accessed=1 << 22, transcendentals=0),
    )(ranges, index, rows, store, panel)


def decoded(ref, codes, i, width):
    q = ref[rows_of(i, width), :]
    return q.astype(jnp.int32).astype(jnp.float32) * codes[pl.ds(i, 1), :]


def merge_kernel(width, owned, *refs):
    *in_refs, out_ref, codes, new = refs
    for n, ref in enumerate(in_refs):
        codes[n] = scale_of(ref[owned * width :, :].astype(jnp.int32))

    @pl.loop(0, owned, unroll=4)
    def _(i):
        total = sum(decoded(ref, codes.at[n], i, width) for n, ref in enumerate(in_refs))
        y, code = encode(total)
        out_ref[rows_of(i, width), :] = y
        new[pl.ds(i, 1), :] = code

    out_ref[owned * width :, :] = new[...].astype(jnp.int32).astype(jnp.int16)


def merge(terms, width, owned):
    length, block = terms[0].shape
    tail = length - owned * width
    whole = pl.BlockSpec(memory_space=pltpu.VMEM)
    return pl.pallas_call(
        functools.partial(merge_kernel, width, owned),
        out_shape=jax.ShapeDtypeStruct((length, block), jnp.int16),
        in_specs=[whole] * len(terms),
        out_specs=whole,
        scratch_shapes=[
            pltpu.VMEM((len(terms), tail, block), jnp.float32),
            pltpu.VMEM((tail, block), jnp.float32),
        ],
        compiler_params=params(6),
        cost_estimate=pl.CostEstimate(
            flops=1 << 28, bytes_accessed=3 * length * width * 2, transcendentals=0
        ),
    )(*terms)


def finish_kernel(owned, parts, *refs):
    count = sum(1 + part[3] for part in parts)
    out_ref = refs[-2 - sum(part[3] for part in parts)]
    total, codes = refs[-1 - sum(part[3] for part in parts)], refs[-sum(part[3] for part in parts) :]
    in_refs = refs[:count]
    block = total.shape[2]

    at, n = 0, 0
    for width, _, _, terms in parts:
        for ref in in_refs[at + 1 : at + 1 + terms]:
            codes[n][...] = scale_of(ref[owned * width :, :].astype(jnp.int32))
            n += 1
        at += 1 + terms

    @pl.loop(0, owned // 2, unroll=2)
    def _(h):
        for k in range(2):
            i = 2 * h + k
            at, n, offset = 0, 0, 0
            for width, first, last, terms in parts:
                y = in_refs[at][i, first:last, :]
                for ref in in_refs[at + 1 : at + 1 + terms]:
                    rows = pl.ds(pl.multiple_of(i * width + first, 16), last - first)
                    y = y + ref[rows, :].astype(jnp.int32).astype(jnp.float32) * codes[n][pl.ds(i, 1), :]
                    n += 1
                total[k, offset : offset + last - first, :] = y
                at, offset = at + 1 + terms, offset + last - first
            out_ref[rows_of(i, block), :] = total[k].T.astype(out_ref.dtype)


def finish(parts, owned, place, spans, earlier):
    arrays, sizes = [], []
    for own, got, first, last in parts:
        arrays += [own, *got]
        sizes.append((own.shape[1], first, last, len(got)))
    block = own.shape[2]
    tail = got[0].shape[0] - owned * own.shape[1]
    specs = [pl.BlockSpec(a.shape, functools.partial(lambda n, i: (0,) * n, a.ndim)) for a in arrays]
    aliases = {}
    if earlier is not None:
        aliases = {len(arrays): 0}
        arrays.append(earlier)
        specs.append(pl.BlockSpec(memory_space=pl.ANY))
    return pl.pallas_call(
        functools.partial(finish_kernel, owned, sizes),
        out_shape=jax.ShapeDtypeStruct((owned * block, LANES * spans), jnp.bfloat16),
        grid=(1,),
        in_specs=specs,
        out_specs=pl.BlockSpec((owned * block, LANES), lambda i: (0, place)),
        scratch_shapes=[pltpu.VMEM((2, LANES, block), jnp.float32)]
        + [pltpu.VMEM((tail, block), jnp.float32)] * sum(size[3] for size in sizes),
        input_output_aliases=aliases,
        compiler_params=params(12),
        cost_estimate=pl.CostEstimate(
            flops=1 << 28, bytes_accessed=1 << 22, transcendentals=0
        ),
    )(*arrays)


def gather(part, devices):
    pieces = []
    for p in range(0, devices, 2):
        near = part if p == 0 else lax.ppermute(part, "row", [(d, d ^ p) for d in range(devices)])
        pieces += [near, lax.ppermute(near, "row", [(d, d ^ 1) for d in range(devices)])]
    return pieces


def plan(count):
    out = []
    for d in range(count - 1, 1, -1):
        right = [(z, z + d) for z in range(count - d)]
        left = [(z, z - d) for z in range(d, count)]
        hop = [(a, a + 1 if b > a else a - 1) for a, b in right + left]
        ends = [b for _, b in (hop if d > 2 else right + left)]
        if len(set(ends)) == len(ends) and count <= 2 * d:
            out.append(("both", d, right + left, lambda z, d=d: jnp.where(z + d < count, z + d, z - d)))
        else:
            out.append(("right", d, right, lambda z, d=d: z + d))
            out.append(("left", d, left, lambda z, d=d: z - d))
    outer = [(z, z ^ 1) for z in range(count) if z ^ 1 < count]
    middle = [(z, z + 1) for z in range(1, count - 1, 2)]
    out.append(("outer", 1, outer, lambda z: z ^ 1))
    if middle:
        middle += [(b, a) for a, b in middle]
        out.append(("middle", 1, middle, lambda z: z + 2 * (z & 1) - 1))
    return out


def shared(kinds):
    return kinds[-1][0] == "middle" and not {a for a, _ in kinds[0][2]} & {a for a, _ in kinds[-1][2]}


def reduce(kinds, messages, width, owned, chunk):
    got = []
    relayed = {}
    if chunk < DIRECT_CHUNKS:
        for n, ((_, d, pairs, _), message) in enumerate(zip(kinds, messages)):
            if n == 0 and shared(kinds):
                pairs = pairs + kinds[-1][2]
            got.append(lax.ppermute(message, "col", pairs))
        return got
    if shared(kinds):
        got.append(lax.ppermute(messages[0], "col", kinds[-1][2]))
    for (name, d, pairs, _), message in zip(kinds, messages):
        if d == 1:
            got.append(lax.ppermute(message, "col", pairs))
            continue
        sides = ("right", "left") if name == "both" else (name,)
        incoming = []
        for side in sides:
            for array in relayed.get((d + 1, side), []):
                if not any(array is a for a in incoming):
                    incoming.append(array)
        if incoming:
            message = merge([message] + incoming, width, owned)
        if d >= 3:
            hops = [(a, a + 1 if b > a else a - 1) for a, b in pairs]
            array = lax.ppermute(message, "col", hops)
            for side in sides:
                relayed.setdefault((d, side), []).append(array)
        else:
            got.append(lax.ppermute(message, "col", pairs))
    return got


def local(features, block_values, row_ptr, block_cols):
    values = block_values[0, 0]
    pointers = row_ptr[0, 0]
    block = values.shape[1]
    row_count, col_count = lax.axis_size("row"), lax.axis_size("col")
    mine = features.shape[0] // block
    total_width = features.shape[1]
    owned = (pointers.shape[0] - 1) // col_count

    kinds = plan(col_count)
    count = len(kinds) - shared(kinds)

    def owner_of(col):
        for n, (_, _, pairs, owner) in enumerate(kinds[:count]):
            there = owner(col)
            if n == 0 and shared(kinds):
                first = sum((col == a).astype(jnp.int32) for a, _ in pairs)
                there = jnp.where(first > 0, there, kinds[-1][3](col))
            yield there
        yield col

    starts = [total_width * sum(CHUNKS[:n]) // sum(CHUNKS) for n in range(len(CHUNKS) + 1)]
    parts = []
    for first, last in zip(starts, starts[1:]):
        piece = turn(features, block, first, last - first)
        parts.append(gather(piece, row_count))
    ranges, index, rows, store = stage(
        pointers, block_cols[0, 0], values, owner_of, count + 1, mine
    )
    sums, written, out = [], 0, None
    for chunk, pieces in enumerate(parts):
        lead, panel = head(ranges, index, rows, store, pieces, owned)
        *others, own = rest(
            ranges, index, rows, store, panel, owned, pointers.shape[0] - 1, count - 1
        )
        got = reduce(kinds, [lead, *others], own.shape[1], owned, chunk)
        sums.append((own, got))
        while written + LANES <= starts[chunk + 1]:
            taken = [
                (*sums[n], max(written - first, 0), min(written + LANES, last) - first)
                for n, (first, last) in enumerate(zip(starts, starts[1:]))
                if first < written + LANES and last > written
            ]
            out = finish(taken, owned, written // LANES, total_width // LANES, out)
            written += LANES
    return out


def solution(mesh):
    return jax.shard_map(
        local,
        mesh=mesh,
        in_specs=(
            P(("col", "row"), None),
            P("row", "col", None, None, None),
            P("row", "col", None),
            P("row", "col", None),
        ),
        out_specs=P(("row", "col"), None),
        check_vma=False,
    )
```

```python
import functools

import jax
import jax.numpy as jnp
from jax import lax
from jax.experimental import pallas as pl
from jax.experimental.pallas import tpu as pltpu
from jax.sharding import PartitionSpec as P


LANES = 128
UNROLL = 16
MIB = 1 << 20
STAGE_MIB = 46
DIRECT_CHUNKS = 1
PASSED_FROM = 2
CHUNKS = (3, 5, 8)
TOP = 32700.0
STEPS = 8.0
TINY = 2.0**-110


def code_of(peak):
    return jnp.ceil(jnp.log2(jnp.maximum(peak, TINY)) * STEPS)


def encode(y):
    code = code_of(jnp.max(jnp.abs(y), axis=0, keepdims=True))
    coded = jnp.round(y * (jnp.exp2(code * (-1.0 / STEPS)) * TOP))
    return coded.astype(jnp.int32).astype(jnp.int16), code


def scale_of(codes):
    return jnp.exp2(codes.astype(jnp.float32) * (1.0 / STEPS)) * (1.0 / TOP)


def rows_of(i, size):
    return pl.ds(pl.multiple_of(i * size, size), size)


def params(mib):
    return pltpu.CompilerParams(vmem_limit_bytes=mib * MIB)


def turn_kernel(block, first, x_ref, out_ref):
    mine, width = out_ref.shape[:2]
    aligned, last = first // LANES * LANES, first + width
    end = -(-last // LANES) * LANES

    @pl.loop(0, mine, unroll=4)
    def _(j):
        y = x_ref[rows_of(j, block), aligned:end].T
        out_ref[j] = y[first - aligned : last - aligned, :]


def turn(features, block, first, width):
    mine = features.shape[0] // block
    whole = pl.BlockSpec(memory_space=pltpu.VMEM)
    return pl.pallas_call(
        functools.partial(turn_kernel, block, first),
        out_shape=jax.ShapeDtypeStruct((mine, width, block), features.dtype),
        in_specs=[whole],
        out_specs=whole,
        compiler_params=params(4),
        cost_estimate=pl.CostEstimate(flops=1 << 26, bytes_accessed=1 << 20, transcendentals=0),
    )(features)


def stage_kernel(
    owner_of, mine, pointer_ref, column_ref, values_ref, range_ref, index_ref, row_ref, store_ref, sem
):
    local_rows = pointer_ref.shape[0] - 1
    slots = column_ref.shape[0]
    row, col = lax.axis_index("row"), lax.axis_index("col")
    group = mine * lax.axis_size("row")
    total = pointer_ref[local_rows]
    steps = (total + UNROLL - 1) // UNROLL

    def copy(t):
        span = pl.ds(t * UNROLL, UNROLL)
        return pltpu.make_async_copy(values_ref.at[span], store_ref.at[span], sem.at[t])

    @pl.loop(0, steps)
    def _(t):
        copy(t).start()

    @pl.loop(0, jnp.minimum(slots // UNROLL, steps + 1))
    def _(t):
        for u in range(UNROLL):
            column = column_ref[t * UNROLL + u] - col * group
            device = lax.div(column, mine)
            index_ref[t * UNROLL + u] = (device ^ row) * mine + column - device * mine

    @pl.loop(0, local_rows)
    def _(i):
        @pl.loop(pointer_ref[i], pointer_ref[i + 1])
        def _(s):
            row_ref[s] = i

    owned = local_rows // lax.axis_size("col")
    for m, owner in enumerate(owner_of(col)):
        first = jnp.clip(owner, 0, lax.axis_size("col") - 1) * owned
        sent = (owner >= 0) & (owner < lax.axis_size("col"))
        range_ref[3 * m] = jnp.where(sent, pointer_ref[first], 0)
        range_ref[3 * m + 1] = jnp.where(sent, pointer_ref[first + owned], 0)
        range_ref[3 * m + 2] = first
    range_ref[3 * m + 3] = total

    @pl.loop(0, steps)
    def _(t):
        copy(t).wait()


def stage(pointers, columns, values, owner_of, count, mine):
    smem = pl.BlockSpec(memory_space=pltpu.SMEM)
    whole = pl.BlockSpec(memory_space=pltpu.VMEM)
    slots = values.shape[0]
    return pl.pallas_call(
        functools.partial(stage_kernel, owner_of, mine),
        out_shape=[
            jax.ShapeDtypeStruct((3 * count + 1,), jnp.int32),
            jax.ShapeDtypeStruct((slots,), jnp.int32),
            jax.ShapeDtypeStruct((slots,), jnp.int32),
            jax.ShapeDtypeStruct(values.shape, values.dtype),
        ],
        in_specs=[smem, smem, pl.BlockSpec(memory_space=pltpu.HBM)],
        out_specs=[smem] * 3 + [whole],
        scratch_shapes=[pltpu.SemaphoreType.DMA((-(-slots // UNROLL),))],
        compiler_params=params(STAGE_MIB),
        cost_estimate=pl.CostEstimate(flops=1 << 26, bytes_accessed=1 << 22, transcendentals=0),
    )(pointers, columns, values)


def add_slots(low, high, spare, offset, index_ref, row_ref, store, panel, acc):
    @pl.loop(0, (high - low + UNROLL - 1) // UNROLL)
    def _(t):
        terms = []
        for u in range(UNROLL):
            s = low + t * UNROLL + u
            terms.append(
                lax.dot_general(
                    panel[index_ref[s]],
                    store[s],
                    (((1,), (1,)), ((), ())),
                    preferred_element_type=jnp.float32,
                )
            )
        for u in range(UNROLL):
            s = low + t * UNROLL + u
            acc[jnp.where(s < high, row_ref[s] - offset, spare)] += terms[u]


def write_message(acc, first, out_ref, codes, owned, width):
    @pl.loop(0, owned, unroll=4)
    def _(i):
        y, code = encode(acc[first + i])
        out_ref[rows_of(i, width), :] = y
        codes[pl.ds(i, 1), :] = code

    out_ref[owned * width :, :] = codes[...].astype(jnp.int32).astype(jnp.int16)


def clear(acc, count):
    @pl.loop(0, count, unroll=4)
    def _(i):
        acc[i] = jnp.zeros(acc.shape[1:], acc.dtype)


def head_kernel(owned, range_ref, index_ref, row_ref, store, *refs):
    *piece_refs, out_ref, panel, acc, codes = refs
    width = panel.shape[1]
    at = 0
    for ref in piece_refs:

        @pl.loop(0, ref.shape[0], unroll=4)
        def _(j):
            panel[at + j] = ref[j]

        at += ref.shape[0]

    clear(acc, owned)
    low, high, first = (range_ref[n] for n in range(3))
    add_slots(low, high, owned, first, index_ref, row_ref, store, panel, acc)
    write_message(acc, 0, out_ref, codes, owned, width)


def rest_kernel(owned, messages, local_rows, range_ref, index_ref, row_ref, store, panel, *refs):
    out_refs = refs[:messages]
    own_ref, acc, codes = refs[messages:]
    width = panel.shape[1]
    clear(acc, local_rows)
    low, high, total = range_ref[0], range_ref[1], range_ref[3 * messages + 6]
    add_slots(0, low, local_rows, 0, index_ref, row_ref, store, panel, acc)
    add_slots(high, total, local_rows, 0, index_ref, row_ref, store, panel, acc)
    for m, out_ref in enumerate(out_refs):
        write_message(acc, range_ref[3 * m + 5], out_ref, codes, owned, width)
    first = range_ref[3 * messages + 5]

    @pl.loop(0, owned, unroll=4)
    def _(i):
        own_ref[i] = acc[first + i]


def head(ranges, index, rows, store, pieces, owned):
    slots, block = store.shape[:2]
    width = pieces[0].shape[1]
    tail = -(-owned // 16) * 16
    smem = pl.BlockSpec(memory_space=pltpu.SMEM)
    whole = pl.BlockSpec(memory_space=pltpu.VMEM)
    flops = slots * block * block * width
    return pl.pallas_call(
        functools.partial(head_kernel, owned),
        out_shape=[
            jax.ShapeDtypeStruct((owned * width + tail, block), jnp.int16),
            jax.ShapeDtypeStruct((sum(p.shape[0] for p in pieces), width, block), store.dtype),
        ],
        in_specs=[smem] * 3 + [whole] * (1 + len(pieces)),
        out_specs=[whole] * 2,
        scratch_shapes=[
            pltpu.VMEM((owned + 1, width, block), jnp.float32),
            pltpu.VMEM((tail, block), jnp.float32),
        ],
        compiler_params=params(10),
        cost_estimate=pl.CostEstimate(flops=flops, bytes_accessed=1 << 22, transcendentals=0),
    )(ranges, index, rows, store, *pieces)


def rest(ranges, index, rows, store, panel, owned, local_rows, messages):
    slots, block = store.shape[:2]
    width = panel.shape[1]
    tail = -(-owned // 16) * 16
    smem = pl.BlockSpec(memory_space=pltpu.SMEM)
    whole = pl.BlockSpec(memory_space=pltpu.VMEM)
    flops = 2 * slots * block * block * width
    return pl.pallas_call(
        functools.partial(rest_kernel, owned, messages, local_rows),
        out_shape=[jax.ShapeDtypeStruct((owned * width + tail, block), jnp.int16)] * messages
        + [jax.ShapeDtypeStruct((owned, width, block), jnp.float32)],
        in_specs=[smem] * 3 + [whole] * 2,
        out_specs=[whole] * (messages + 1),
        scratch_shapes=[
            pltpu.VMEM((local_rows + 1, width, block), jnp.float32),
            pltpu.VMEM((tail, block), jnp.float32),
        ],
        compiler_params=params(12),
        cost_estimate=pl.CostEstimate(flops=flops, bytes_accessed=1 << 22, transcendentals=0),
    )(ranges, index, rows, store, panel)


def decoded(ref, codes, i, width):
    q = ref[rows_of(i, width), :]
    return q.astype(jnp.int32).astype(jnp.float32) * codes[pl.ds(i, 1), :]


def merge_kernel(width, owned, *refs):
    *in_refs, out_ref, codes, new = refs
    for n, ref in enumerate(in_refs):
        codes[n] = scale_of(ref[owned * width :, :].astype(jnp.int32))

    @pl.loop(0, owned, unroll=4)
    def _(i):
        total = sum(decoded(ref, codes.at[n], i, width) for n, ref in enumerate(in_refs))
        y, code = encode(total)
        out_ref[rows_of(i, width), :] = y
        new[pl.ds(i, 1), :] = code

    out_ref[owned * width :, :] = new[...].astype(jnp.int32).astype(jnp.int16)


def merge(terms, width, owned):
    length, block = terms[0].shape
    tail = length - owned * width
    whole = pl.BlockSpec(memory_space=pltpu.VMEM)
    return pl.pallas_call(
        functools.partial(merge_kernel, width, owned),
        out_shape=jax.ShapeDtypeStruct((length, block), jnp.int16),
        in_specs=[whole] * len(terms),
        out_specs=whole,
        scratch_shapes=[
            pltpu.VMEM((len(terms), tail, block), jnp.float32),
            pltpu.VMEM((tail, block), jnp.float32),
        ],
        compiler_params=params(6),
        cost_estimate=pl.CostEstimate(
            flops=1 << 28, bytes_accessed=3 * length * width * 2, transcendentals=0
        ),
    )(*terms)


def finish_kernel(owned, parts, *refs):
    count = sum(1 + part[3] for part in parts)
    out_ref = refs[-2 - sum(part[3] for part in parts)]
    total, codes = refs[-1 - sum(part[3] for part in parts)], refs[-sum(part[3] for part in parts) :]
    in_refs = refs[:count]
    block = total.shape[2]

    at, n = 0, 0
    for width, _, _, terms in parts:
        for ref in in_refs[at + 1 : at + 1 + terms]:
            codes[n][...] = scale_of(ref[owned * width :, :].astype(jnp.int32))
            n += 1
        at += 1 + terms

    @pl.loop(0, owned // 2, unroll=2)
    def _(h):
        for k in range(2):
            i = 2 * h + k
            at, n, offset = 0, 0, 0
            for width, first, last, terms in parts:
                y = in_refs[at][i, first:last, :]
                for ref in in_refs[at + 1 : at + 1 + terms]:
                    rows = pl.ds(pl.multiple_of(i * width + first, 16), last - first)
                    y = y + ref[rows, :].astype(jnp.int32).astype(jnp.float32) * codes[n][pl.ds(i, 1), :]
                    n += 1
                total[k, offset : offset + last - first, :] = y
                at, offset = at + 1 + terms, offset + last - first
            out_ref[rows_of(i, block), :] = total[k].T.astype(out_ref.dtype)


def finish(parts, owned, place, spans, earlier):
    arrays, sizes = [], []
    for own, got, first, last in parts:
        arrays += [own, *got]
        sizes.append((own.shape[1], first, last, len(got)))
    block = own.shape[2]
    tail = got[0].shape[0] - owned * own.shape[1]
    specs = [pl.BlockSpec(a.shape, functools.partial(lambda n, i: (0,) * n, a.ndim)) for a in arrays]
    aliases = {}
    if earlier is not None:
        aliases = {len(arrays): 0}
        arrays.append(earlier)
        specs.append(pl.BlockSpec(memory_space=pl.ANY))
    return pl.pallas_call(
        functools.partial(finish_kernel, owned, sizes),
        out_shape=jax.ShapeDtypeStruct((owned * block, LANES * spans), jnp.bfloat16),
        grid=(1,),
        in_specs=specs,
        out_specs=pl.BlockSpec((owned * block, LANES), lambda i: (0, place)),
        scratch_shapes=[pltpu.VMEM((2, LANES, block), jnp.float32)]
        + [pltpu.VMEM((tail, block), jnp.float32)] * sum(size[3] for size in sizes),
        input_output_aliases=aliases,
        compiler_params=params(12),
        cost_estimate=pl.CostEstimate(
            flops=1 << 28, bytes_accessed=1 << 22, transcendentals=0
        ),
    )(*arrays)


def gather(part, devices, passed):
    def swap(array, bits):
        return lax.ppermute(array, "row", [(d, d ^ bits) for d in range(devices)])

    near = {0: [part]}
    for p in range(2, devices, 2):
        low = p & -p
        if passed and p != low and (p ^ low) & ((p ^ low) - 1) == 0:
            half = part.shape[0] // 2
            near[p] = [swap(near[p ^ low][0][:half], low), swap(near[low][0][half:], p ^ low)]
        else:
            near[p] = [swap(part, p)]
    pieces = []
    for arrays in near.values():
        pieces += [*arrays, *(swap(array, 1) for array in arrays)]
    return pieces


def plan(count):
    out = []
    for d in range(count - 1, 1, -1):
        right = [(z, z + d) for z in range(count - d)]
        left = [(z, z - d) for z in range(d, count)]
        hop = [(a, a + 1 if b > a else a - 1) for a, b in right + left]
        ends = [b for _, b in (hop if d > 2 else right + left)]
        if len(set(ends)) == len(ends) and count <= 2 * d:
            out.append(("both", d, right + left, lambda z, d=d: jnp.where(z + d < count, z + d, z - d)))
        else:
            out.append(("right", d, right, lambda z, d=d: z + d))
            out.append(("left", d, left, lambda z, d=d: z - d))
    outer = [(z, z ^ 1) for z in range(count) if z ^ 1 < count]
    middle = [(z, z + 1) for z in range(1, count - 1, 2)]
    out.append(("outer", 1, outer, lambda z: z ^ 1))
    if middle:
        middle += [(b, a) for a, b in middle]
        out.append(("middle", 1, middle, lambda z: z + 2 * (z & 1) - 1))
    return out


def shared(kinds):
    return kinds[-1][0] == "middle" and not {a for a, _ in kinds[0][2]} & {a for a, _ in kinds[-1][2]}


def reduce(kinds, messages, width, owned, chunk):
    got = []
    relayed = {}
    if chunk < DIRECT_CHUNKS:
        for n, ((_, d, pairs, _), message) in enumerate(zip(kinds, messages)):
            if n == 0 and shared(kinds):
                pairs = pairs + kinds[-1][2]
            got.append(lax.ppermute(message, "col", pairs))
        return got
    if shared(kinds):
        got.append(lax.ppermute(messages[0], "col", kinds[-1][2]))
    for (name, d, pairs, _), message in zip(kinds, messages):
        if d == 1:
            got.append(lax.ppermute(message, "col", pairs))
            continue
        sides = ("right", "left") if name == "both" else (name,)
        incoming = []
        for side in sides:
            for array in relayed.get((d + 1, side), []):
                if not any(array is a for a in incoming):
                    incoming.append(array)
        if incoming:
            message = merge([message] + incoming, width, owned)
        if d >= 3:
            hops = [(a, a + 1 if b > a else a - 1) for a, b in pairs]
            array = lax.ppermute(message, "col", hops)
            for side in sides:
                relayed.setdefault((d, side), []).append(array)
        else:
            got.append(lax.ppermute(message, "col", pairs))
    return got


def local(features, block_values, row_ptr, block_cols):
    values = block_values[0, 0]
    pointers = row_ptr[0, 0]
    block = values.shape[1]
    row_count, col_count = lax.axis_size("row"), lax.axis_size("col")
    mine = features.shape[0] // block
    total_width = features.shape[1]
    owned = (pointers.shape[0] - 1) // col_count

    kinds = plan(col_count)
    count = len(kinds) - shared(kinds)

    def owner_of(col):
        for n, (_, _, pairs, owner) in enumerate(kinds[:count]):
            there = owner(col)
            if n == 0 and shared(kinds):
                first = sum((col == a).astype(jnp.int32) for a, _ in pairs)
                there = jnp.where(first > 0, there, kinds[-1][3](col))
            yield there
        yield col

    starts = [total_width * sum(CHUNKS[:n]) // sum(CHUNKS) for n in range(len(CHUNKS) + 1)]
    parts = []
    for chunk, (first, last) in enumerate(zip(starts, starts[1:])):
        piece = turn(features, block, first, last - first)
        parts.append(gather(piece, row_count, chunk >= PASSED_FROM))
    ranges, index, rows, store = stage(
        pointers, block_cols[0, 0], values, owner_of, count + 1, mine
    )
    sums, written, out = [], 0, None
    for chunk, pieces in enumerate(parts):
        lead, panel = head(ranges, index, rows, store, pieces, owned)
        *others, own = rest(
            ranges, index, rows, store, panel, owned, pointers.shape[0] - 1, count - 1
        )
        got = reduce(kinds, [lead, *others], own.shape[1], owned, chunk)
        sums.append((own, got))
        while written + LANES <= starts[chunk + 1]:
            taken = [
                (*sums[n], max(written - first, 0), min(written + LANES, last) - first)
                for n, (first, last) in enumerate(zip(starts, starts[1:]))
                if first < written + LANES and last > written
            ]
            out = finish(taken, owned, written // LANES, total_width // LANES, out)
            written += LANES
    return out


def solution(mesh):
    return jax.shard_map(
        local,
        mesh=mesh,
        in_specs=(
            P(("col", "row"), None),
            P("row", "col", None, None, None),
            P("row", "col", None),
            P("row", "col", None),
        ),
        out_specs=P(("row", "col"), None),
        check_vma=False,
    )
```

```python
import functools

import jax
import jax.numpy as jnp
from jax import lax
from jax.experimental import pallas as pl
from jax.experimental.pallas import tpu as pltpu
from jax.sharding import PartitionSpec as P


LANES = 128
UNROLL = 16
MIB = 1 << 20
STAGE_MIB = 46
DIRECT_CHUNKS = 1
PASSED_FROM = 2
CHUNKS = (3, 5, 8)
TOP = 32700.0
STEPS = 8.0
TINY = 2.0**-110


def code_of(peak):
    return jnp.ceil(jnp.log2(jnp.maximum(peak, TINY)) * STEPS)


def encode(y):
    code = code_of(jnp.max(jnp.abs(y), axis=0, keepdims=True))
    coded = jnp.round(y * (jnp.exp2(code * (-1.0 / STEPS)) * TOP))
    return coded.astype(jnp.int32).astype(jnp.int16), code


def scale_of(codes):
    return jnp.exp2(codes.astype(jnp.float32) * (1.0 / STEPS)) * (1.0 / TOP)


def rows_of(i, size):
    return pl.ds(pl.multiple_of(i * size, size), size)


def params(mib):
    return pltpu.CompilerParams(vmem_limit_bytes=mib * MIB)


def turn_kernel(block, first, x_ref, out_ref):
    mine, width = out_ref.shape[:2]
    aligned, last = first // LANES * LANES, first + width
    end = -(-last // LANES) * LANES

    @pl.loop(0, mine, unroll=4)
    def _(j):
        y = x_ref[rows_of(j, block), aligned:end].T
        out_ref[j] = y[first - aligned : last - aligned, :]


def turn(features, block, first, width):
    mine = features.shape[0] // block
    whole = pl.BlockSpec(memory_space=pltpu.VMEM)
    return pl.pallas_call(
        functools.partial(turn_kernel, block, first),
        out_shape=jax.ShapeDtypeStruct((mine, width, block), features.dtype),
        in_specs=[whole],
        out_specs=whole,
        compiler_params=params(4),
        cost_estimate=pl.CostEstimate(flops=1 << 26, bytes_accessed=1 << 20, transcendentals=0),
    )(features)


def stage_kernel(
    owner_of, mine, pointer_ref, column_ref, values_ref, range_ref, index_ref, row_ref, store_ref, sem
):
    local_rows = pointer_ref.shape[0] - 1
    slots = column_ref.shape[0]
    row, col = lax.axis_index("row"), lax.axis_index("col")
    group = mine * lax.axis_size("row")
    total = pointer_ref[local_rows]
    steps = (total + UNROLL - 1) // UNROLL

    def copy(t):
        span = pl.ds(t * UNROLL, UNROLL)
        return pltpu.make_async_copy(values_ref.at[span], store_ref.at[span], sem.at[t])

    @pl.loop(0, steps)
    def _(t):
        copy(t).start()

    @pl.loop(0, jnp.minimum(slots // UNROLL, steps + 1))
    def _(t):
        for u in range(UNROLL):
            column = column_ref[t * UNROLL + u] - col * group
            device = lax.div(column, mine)
            index_ref[t * UNROLL + u] = (device ^ row) * mine + column - device * mine

    @pl.loop(0, local_rows)
    def _(i):
        @pl.loop(pointer_ref[i], pointer_ref[i + 1])
        def _(s):
            row_ref[s] = i

    owned = local_rows // lax.axis_size("col")
    for m, owner in enumerate(owner_of(col)):
        first = jnp.clip(owner, 0, lax.axis_size("col") - 1) * owned
        sent = (owner >= 0) & (owner < lax.axis_size("col"))
        range_ref[3 * m] = jnp.where(sent, pointer_ref[first], 0)
        range_ref[3 * m + 1] = jnp.where(sent, pointer_ref[first + owned], 0)
        range_ref[3 * m + 2] = first
    range_ref[3 * m + 3] = total

    @pl.loop(0, steps)
    def _(t):
        copy(t).wait()


def stage(pointers, columns, values, owner_of, count, mine):
    smem = pl.BlockSpec(memory_space=pltpu.SMEM)
    whole = pl.BlockSpec(memory_space=pltpu.VMEM)
    slots = values.shape[0]
    return pl.pallas_call(
        functools.partial(stage_kernel, owner_of, mine),
        out_shape=[
            jax.ShapeDtypeStruct((3 * count + 1,), jnp.int32),
            jax.ShapeDtypeStruct((slots,), jnp.int32),
            jax.ShapeDtypeStruct((slots,), jnp.int32),
            jax.ShapeDtypeStruct(values.shape, values.dtype),
        ],
        in_specs=[smem, smem, pl.BlockSpec(memory_space=pltpu.HBM)],
        out_specs=[smem] * 3 + [whole],
        scratch_shapes=[pltpu.SemaphoreType.DMA((-(-slots // UNROLL),))],
        compiler_params=params(STAGE_MIB),
        cost_estimate=pl.CostEstimate(flops=1 << 26, bytes_accessed=1 << 22, transcendentals=0),
    )(pointers, columns, values)


def add_slots(low, high, spare, offset, index_ref, row_ref, store, panel, acc):
    @pl.loop(0, (high - low + UNROLL - 1) // UNROLL)
    def _(t):
        terms = []
        for u in range(UNROLL):
            s = low + t * UNROLL + u
            terms.append(
                lax.dot_general(
                    panel[index_ref[s]],
                    store[s],
                    (((1,), (1,)), ((), ())),
                    preferred_element_type=jnp.float32,
                )
            )
        for u in range(UNROLL):
            s = low + t * UNROLL + u
            acc[jnp.where(s < high, row_ref[s] - offset, spare)] += terms[u]


def write_message(acc, first, out_ref, codes, owned, width):
    @pl.loop(0, owned, unroll=min(8, owned))
    def _(i):
        y, code = encode(acc[first + i])
        out_ref[rows_of(i, width), :] = y
        codes[pl.ds(i, 1), :] = code

    out_ref[owned * width :, :] = codes[...].astype(jnp.int32).astype(jnp.int16)


def clear(acc, count):
    @pl.loop(0, count, unroll=4)
    def _(i):
        acc[i] = jnp.zeros(acc.shape[1:], acc.dtype)


def head_kernel(owned, range_ref, index_ref, row_ref, store, *refs):
    *piece_refs, out_ref, panel, acc, codes = refs
    width = panel.shape[1]
    at = 0
    for ref in piece_refs:

        @pl.loop(0, ref.shape[0], unroll=min(8, ref.shape[0]))
        def _(j):
            panel[at + j] = ref[j]

        at += ref.shape[0]

    clear(acc, owned)
    low, high, first = (range_ref[n] for n in range(3))
    add_slots(low, high, owned, first, index_ref, row_ref, store, panel, acc)
    write_message(acc, 0, out_ref, codes, owned, width)


def rest_kernel(owned, messages, local_rows, range_ref, index_ref, row_ref, store, panel, *refs):
    out_refs = refs[:messages]
    own_ref, acc, codes = refs[messages:]
    width = panel.shape[1]
    clear(acc, local_rows)
    low, high, total = range_ref[0], range_ref[1], range_ref[3 * messages + 6]
    add_slots(0, low, local_rows, 0, index_ref, row_ref, store, panel, acc)
    add_slots(high, total, local_rows, 0, index_ref, row_ref, store, panel, acc)
    for m, out_ref in enumerate(out_refs):
        write_message(acc, range_ref[3 * m + 5], out_ref, codes, owned, width)
    first = range_ref[3 * messages + 5]

    @pl.loop(0, owned, unroll=4)
    def _(i):
        own_ref[i] = acc[first + i]


def head(ranges, index, rows, store, pieces, owned):
    slots, block = store.shape[:2]
    width = pieces[0].shape[1]
    tail = -(-owned // 16) * 16
    smem = pl.BlockSpec(memory_space=pltpu.SMEM)
    whole = pl.BlockSpec(memory_space=pltpu.VMEM)
    flops = slots * block * block * width
    return pl.pallas_call(
        functools.partial(head_kernel, owned),
        out_shape=[
            jax.ShapeDtypeStruct((owned * width + tail, block), jnp.int16),
            jax.ShapeDtypeStruct((sum(p.shape[0] for p in pieces), width, block), store.dtype),
        ],
        in_specs=[smem] * 3 + [whole] * (1 + len(pieces)),
        out_specs=[whole] * 2,
        scratch_shapes=[
            pltpu.VMEM((owned + 1, width, block), jnp.float32),
            pltpu.VMEM((tail, block), jnp.float32),
        ],
        compiler_params=params(10),
        cost_estimate=pl.CostEstimate(flops=flops, bytes_accessed=1 << 22, transcendentals=0),
    )(ranges, index, rows, store, *pieces)


def rest(ranges, index, rows, store, panel, owned, local_rows, messages):
    slots, block = store.shape[:2]
    width = panel.shape[1]
    tail = -(-owned // 16) * 16
    smem = pl.BlockSpec(memory_space=pltpu.SMEM)
    whole = pl.BlockSpec(memory_space=pltpu.VMEM)
    flops = 2 * slots * block * block * width
    return pl.pallas_call(
        functools.partial(rest_kernel, owned, messages, local_rows),
        out_shape=[jax.ShapeDtypeStruct((owned * width + tail, block), jnp.int16)] * messages
        + [jax.ShapeDtypeStruct((owned, width, block), jnp.float32)],
        in_specs=[smem] * 3 + [whole] * 2,
        out_specs=[whole] * (messages + 1),
        scratch_shapes=[
            pltpu.VMEM((local_rows + 1, width, block), jnp.float32),
            pltpu.VMEM((tail, block), jnp.float32),
        ],
        compiler_params=params(12),
        cost_estimate=pl.CostEstimate(flops=flops, bytes_accessed=1 << 22, transcendentals=0),
    )(ranges, index, rows, store, panel)


def decoded(ref, codes, i, width):
    q = ref[rows_of(i, width), :]
    return q.astype(jnp.int32).astype(jnp.float32) * codes[pl.ds(i, 1), :]


def merge_kernel(width, owned, *refs):
    *in_refs, out_ref, codes, new = refs
    for n, ref in enumerate(in_refs):
        codes[n] = scale_of(ref[owned * width :, :].astype(jnp.int32))

    @pl.loop(0, owned, unroll=4)
    def _(i):
        total = sum(decoded(ref, codes.at[n], i, width) for n, ref in enumerate(in_refs))
        y, code = encode(total)
        out_ref[rows_of(i, width), :] = y
        new[pl.ds(i, 1), :] = code

    out_ref[owned * width :, :] = new[...].astype(jnp.int32).astype(jnp.int16)


def merge(terms, width, owned):
    length, block = terms[0].shape
    tail = length - owned * width
    whole = pl.BlockSpec(memory_space=pltpu.VMEM)
    return pl.pallas_call(
        functools.partial(merge_kernel, width, owned),
        out_shape=jax.ShapeDtypeStruct((length, block), jnp.int16),
        in_specs=[whole] * len(terms),
        out_specs=whole,
        scratch_shapes=[
            pltpu.VMEM((len(terms), tail, block), jnp.float32),
            pltpu.VMEM((tail, block), jnp.float32),
        ],
        compiler_params=params(6),
        cost_estimate=pl.CostEstimate(
            flops=1 << 28, bytes_accessed=3 * length * width * 2, transcendentals=0
        ),
    )(*terms)


def finish_kernel(owned, parts, *refs):
    count = sum(1 + part[3] for part in parts)
    out_ref = refs[-2 - sum(part[3] for part in parts)]
    total, codes = refs[-1 - sum(part[3] for part in parts)], refs[-sum(part[3] for part in parts) :]
    in_refs = refs[:count]
    block = total.shape[2]

    at, n = 0, 0
    for width, _, _, terms in parts:
        for ref in in_refs[at + 1 : at + 1 + terms]:
            codes[n][...] = scale_of(ref[owned * width :, :].astype(jnp.int32))
            n += 1
        at += 1 + terms

    @pl.loop(0, owned // 2, unroll=min(4, owned // 2))
    def _(h):
        for k in range(2):
            i = 2 * h + k
            at, n, offset = 0, 0, 0
            for width, first, last, terms in parts:
                y = in_refs[at][i, first:last, :]
                for ref in in_refs[at + 1 : at + 1 + terms]:
                    rows = pl.ds(pl.multiple_of(i * width + first, 16), last - first)
                    y = y + ref[rows, :].astype(jnp.int32).astype(jnp.float32) * codes[n][pl.ds(i, 1), :]
                    n += 1
                total[k, offset : offset + last - first, :] = y
                at, offset = at + 1 + terms, offset + last - first
            out_ref[rows_of(i, block), :] = total[k].T.astype(out_ref.dtype)


def finish(parts, owned, place, spans, earlier):
    arrays, sizes = [], []
    for own, got, first, last in parts:
        arrays += [own, *got]
        sizes.append((own.shape[1], first, last, len(got)))
    block = own.shape[2]
    tail = got[0].shape[0] - owned * own.shape[1]
    specs = [pl.BlockSpec(a.shape, functools.partial(lambda n, i: (0,) * n, a.ndim)) for a in arrays]
    aliases = {}
    if earlier is not None:
        aliases = {len(arrays): 0}
        arrays.append(earlier)
        specs.append(pl.BlockSpec(memory_space=pl.ANY))
    return pl.pallas_call(
        functools.partial(finish_kernel, owned, sizes),
        out_shape=jax.ShapeDtypeStruct((owned * block, LANES * spans), jnp.bfloat16),
        grid=(1,),
        in_specs=specs,
        out_specs=pl.BlockSpec((owned * block, LANES), lambda i: (0, place)),
        scratch_shapes=[pltpu.VMEM((2, LANES, block), jnp.float32)]
        + [pltpu.VMEM((tail, block), jnp.float32)] * sum(size[3] for size in sizes),
        input_output_aliases=aliases,
        compiler_params=params(12),
        cost_estimate=pl.CostEstimate(
            flops=1 << 28, bytes_accessed=1 << 22, transcendentals=0
        ),
    )(*arrays)


def gather(part, devices, passed):
    def swap(array, bits):
        return lax.ppermute(array, "row", [(d, d ^ bits) for d in range(devices)])

    near = {0: [part]}
    for p in range(2, devices, 2):
        low = p & -p
        if passed and p != low and (p ^ low) & ((p ^ low) - 1) == 0:
            half = part.shape[0] // 2
            near[p] = [swap(near[p ^ low][0][:half], low), swap(near[low][0][half:], p ^ low)]
        else:
            near[p] = [swap(part, p)]
    pieces = []
    for arrays in near.values():
        pieces += [*arrays, *(swap(array, 1) for array in arrays)]
    return pieces


def plan(count):
    out = []
    for d in range(count - 1, 1, -1):
        right = [(z, z + d) for z in range(count - d)]
        left = [(z, z - d) for z in range(d, count)]
        hop = [(a, a + 1 if b > a else a - 1) for a, b in right + left]
        ends = [b for _, b in (hop if d > 2 else right + left)]
        if len(set(ends)) == len(ends) and count <= 2 * d:
            out.append(("both", d, right + left, lambda z, d=d: jnp.where(z + d < count, z + d, z - d)))
        else:
            out.append(("right", d, right, lambda z, d=d: z + d))
            out.append(("left", d, left, lambda z, d=d: z - d))
    outer = [(z, z ^ 1) for z in range(count) if z ^ 1 < count]
    middle = [(z, z + 1) for z in range(1, count - 1, 2)]
    out.append(("outer", 1, outer, lambda z: z ^ 1))
    if middle:
        middle += [(b, a) for a, b in middle]
        out.append(("middle", 1, middle, lambda z: z + 2 * (z & 1) - 1))
    return out


def shared(kinds):
    return kinds[-1][0] == "middle" and not {a for a, _ in kinds[0][2]} & {a for a, _ in kinds[-1][2]}


def reduce(kinds, messages, width, owned, chunk):
    got = []
    relayed = {}
    if chunk < DIRECT_CHUNKS:
        for n, ((_, d, pairs, _), message) in enumerate(zip(kinds, messages)):
            if n == 0 and shared(kinds):
                pairs = pairs + kinds[-1][2]
            got.append(lax.ppermute(message, "col", pairs))
        return got
    if shared(kinds):
        got.append(lax.ppermute(messages[0], "col", kinds[-1][2]))
    for (name, d, pairs, _), message in zip(kinds, messages):
        if d == 1:
            got.append(lax.ppermute(message, "col", pairs))
            continue
        sides = ("right", "left") if name == "both" else (name,)
        incoming = []
        for side in sides:
            for array in relayed.get((d + 1, side), []):
                if not any(array is a for a in incoming):
                    incoming.append(array)
        if incoming:
            message = merge([message] + incoming, width, owned)
        if d >= 3:
            hops = [(a, a + 1 if b > a else a - 1) for a, b in pairs]
            array = lax.ppermute(message, "col", hops)
            for side in sides:
                relayed.setdefault((d, side), []).append(array)
        else:
            got.append(lax.ppermute(message, "col", pairs))
    return got


def local(features, block_values, row_ptr, block_cols):
    values = block_values[0, 0]
    pointers = row_ptr[0, 0]
    block = values.shape[1]
    row_count, col_count = lax.axis_size("row"), lax.axis_size("col")
    mine = features.shape[0] // block
    total_width = features.shape[1]
    owned = (pointers.shape[0] - 1) // col_count

    kinds = plan(col_count)
    count = len(kinds) - shared(kinds)

    def owner_of(col):
        for n, (_, _, pairs, owner) in enumerate(kinds[:count]):
            there = owner(col)
            if n == 0 and shared(kinds):
                first = sum((col == a).astype(jnp.int32) for a, _ in pairs)
                there = jnp.where(first > 0, there, kinds[-1][3](col))
            yield there
        yield col

    starts = [total_width * sum(CHUNKS[:n]) // sum(CHUNKS) for n in range(len(CHUNKS) + 1)]
    parts = []
    for chunk, (first, last) in enumerate(zip(starts, starts[1:])):
        piece = turn(features, block, first, last - first)
        parts.append(gather(piece, row_count, chunk >= PASSED_FROM))
    ranges, index, rows, store = stage(
        pointers, block_cols[0, 0], values, owner_of, count + 1, mine
    )
    sums, written, out = [], 0, None
    for chunk, pieces in enumerate(parts):
        lead, panel = head(ranges, index, rows, store, pieces, owned)
        *others, own = rest(
            ranges, index, rows, store, panel, owned, pointers.shape[0] - 1, count - 1
        )
        got = reduce(kinds, [lead, *others], own.shape[1], owned, chunk)
        sums.append((own, got))
        while written + LANES <= starts[chunk + 1]:
            taken = [
                (*sums[n], max(written - first, 0), min(written + LANES, last) - first)
                for n, (first, last) in enumerate(zip(starts, starts[1:]))
                if first < written + LANES and last > written
            ]
            out = finish(taken, owned, written // LANES, total_width // LANES, out)
            written += LANES
    return out


def solution(mesh):
    return jax.shard_map(
        local,
        mesh=mesh,
        in_specs=(
            P(("col", "row"), None),
            P("row", "col", None, None, None),
            P("row", "col", None),
            P("row", "col", None),
        ),
        out_specs=P(("row", "col"), None),
        check_vma=False,
    )
```
